512 devices in a mesh: chan: 2 (over y), row: 128 (over z, x), col: 2 (over core).
Axes of the slice: x: 8, y: 2, z: 16, core: 2. Of those that a mesh axis runs over, the one named last changes fastest.
The devices are a block of a 8x16x16 slice.
Arguments:
- hamiltonian_rows: float32 [256, 2, 2, 65536], P('chan', 'col', None, 'row'), parts along dimension 0, may hold values from -2 to 2, as said below
- current_block: float32 [131072, 256], P(('chan', 'row', 'col')), parts along dimension 0, may hold values from -6 to 6
- correction_block: float32 [131072, 256], P(('chan', 'row', 'col')), parts along dimension 0, may hold values from -6 to 6
- previous_block: float32 [131072, 256], P(('chan', 'row', 'col')), parts along dimension 0, may hold values from -6 to 6
- ritz_values: float32 [512], P('chan'), parts along dimension 0, may hold values from -2 to 2
- mixing_coeffs: float32 [1536, 256], P('chan'), parts along dimension 0, may hold values from -0.21875 to 0.21875
Outputs:
- next_block: float32 [1024, 256], P(('chan', 'row', 'col')), parts along dimension 0
- next_direction: float32 [1024, 256], P(('chan', 'row', 'col')), parts along dimension 0
- next_correction: float32 [1024, 256], P(('chan', 'row', 'col')), parts along dimension 0
- ritz_matrix: float32 [512, 256], P('chan'), parts along dimension 0
- metric_matrix: float32 [512, 256], P('chan'), parts along dimension 0
The draws below stay inside these ranges and needn't reach their ends.
There are 2 independent parts, one for each index of `chan`. The reference program is written for one: setup_inputs(seed, part) draws one part's arguments, and reference() takes and returns one part's arrays. A program takes and returns all parts, laid end to end along the dimension named above; each array names one. Nothing has to cross between parts.
Inputs may be any that keep to these rules, and one draw needn't show every extreme that they name: hamiltonian_rows[a, b, j, :] is row (a * 2 + b) * 256 + j of the channel's Hamiltonian; its entry in that row's own column is the onsite energy.
All inputs are finite; a program needn't handle non-finite values.
Results may differ from the reference program's by a relative error of at most 0.00008.
Values sent between devices are 32-bit elements; how exact they have to be, the bound alone decides.
No kernel may reach another device: no remote copies, remote signals or barrier semaphores. Data moves between devices by JAX's collectives and lax.ppermute only.
A program may use at most 64 MiB of HBM per device.

```python
import math
import jax
import jax.numpy as jnp
from jax import lax

N = 65536
BLOCK = 256
OUT_DEV = 2
N_ROW = 128
N_COL = 2


def draw_hamiltonian_rows(key, part):
    first_key = jax.random.fold_in(key, 11)
    second_key = jax.random.fold_in(key, 12)
    shape = (N_ROW, N_COL, OUT_DEV, N)
    coupling = jax.random.truncated_normal(first_key, -6.0, 6.0, shape, jnp.float32) / math.sqrt(N)
    block_index = lax.broadcasted_iota(jnp.int32, shape, 0) * N_COL + lax.broadcasted_iota(jnp.int32, shape, 1)
    slot_index = lax.broadcasted_iota(jnp.int32, shape, 2)
    column_index = lax.broadcasted_iota(jnp.int32, shape, 3)
    position = (block_index * OUT_DEV + slot_index).astype(jnp.float32) / (N_ROW * N_COL * OUT_DEV)
    row_scale = jnp.exp(position * math.log(3.0))
    onsite = jax.random.uniform(second_key, (N_ROW, N_COL, OUT_DEV, 1), jnp.float32, -2.0, 2.0)
    own_column = column_index == block_index * (N // (N_ROW * N_COL)) + slot_index
    return jnp.where(own_column, onsite, coupling * row_scale)


def block_scale(rng, dims, cuts, smallest, largest):
    def one(dim, blocks):
        heights = jax.random.uniform(jax.random.fold_in(jax.random.fold_in(rng, 6), dim), (blocks,), jnp.float32, smallest / len(cuts), largest / len(cuts))
        return jnp.repeat(jnp.exp(heights), dims[dim] // blocks).reshape((-1,) + (1,) * (len(dims) - dim - 1))

    factor_of = one(*cuts[0])
    for cut in cuts[1:]:
        factor_of = factor_of * one(*cut)
    return factor_of


def normal_values(rng, shape, deviation, limit, cuts=(), held_as=jnp.bfloat16):
    entries = deviation * jax.random.normal(rng, shape, jnp.float32)
    if cuts:
        entries = entries * block_scale(rng, shape, cuts, -0.22, 0.18)
    return jnp.clip(entries, -limit, limit).astype(held_as)


def setup_inputs(seed: int = 0, part: int = 0) -> dict:
    keys = jax.random.split(jax.random.key(seed), 7)
    own_keys = jax.random.split(jax.random.fold_in(keys[6], part), 7)
    return {
        "hamiltonian_rows": draw_hamiltonian_rows(jax.random.fold_in(jax.random.fold_in(keys[6], part), 71), part),
        "current_block": normal_values(own_keys[1], (N, BLOCK), 1.0, 6.0, ((0, 256),), jnp.float32),
        "correction_block": normal_values(own_keys[2], (N, BLOCK), 1.0, 6.0, ((0, 256),), jnp.float32),
        "previous_block": normal_values(own_keys[3], (N, BLOCK), 1.0, 6.0, ((0, 256),), jnp.float32),
        "ritz_values": jnp.clip(jax.random.uniform(own_keys[4], (BLOCK,), jnp.float32, -2.0, 2.0), -2.0, 2.0),
        "mixing_coeffs": normal_values(own_keys[5], (3 * BLOCK, BLOCK), (3 * BLOCK) ** -0.5, 0.21875, (), jnp.float32),
    }


def matmul(left, right):
    return jnp.dot(left, right, preferred_element_type=jnp.float32, precision=lax.Precision.HIGHEST)

def tmatmul(left, right):
    return lax.dot_general(left, right, (((0,), (0,)), ((), ())), preferred_element_type=jnp.float32, precision=lax.Precision.HIGHEST)

def reference(hamiltonian_rows, current_block, correction_block, previous_block, ritz_values, mixing_coeffs):
    blocks = N_ROW * N_COL
    shard_rows = N // blocks
    whole_basis = jnp.concatenate([current_block, correction_block, previous_block], axis=1)
    window_rows = whole_basis.reshape(blocks, shard_rows, 3 * BLOCK)[:, :OUT_DEV, :].reshape(blocks * OUT_DEV, 3 * BLOCK)
    row_tile = hamiltonian_rows.reshape(blocks * OUT_DEV, N)
    product_rows = matmul(row_tile, whole_basis)
    residual = product_rows[:, :BLOCK] - window_rows[:, :BLOCK] * ritz_values[None, :]
    squares = lax.optimization_barrier(jnp.sum(residual * residual, axis=0))
    next_correction = residual * lax.rsqrt(squares / (blocks * OUT_DEV) + 1e-06)
    gram_basis = tmatmul(window_rows, window_rows)
    gram_product = tmatmul(window_rows, product_rows)
    next_block = matmul(window_rows, mixing_coeffs)
    next_direction = matmul(window_rows[:, BLOCK:], mixing_coeffs[BLOCK:, :])
    ritz_matrix = tmatmul(mixing_coeffs, matmul(gram_product, mixing_coeffs))
    metric_matrix = tmatmul(mixing_coeffs, matmul(gram_basis, mixing_coeffs))
    return (next_block, next_direction, next_correction, ritz_matrix, metric_matrix)
```

```python
import jax
import jax.numpy as jnp
from jax import lax
from jax.sharding import Mesh
from jax.sharding import PartitionSpec as P

ROW = ("row_0", "row_1")
CHAN_ROW_COL = ("chan", "row_0", "row_1", "col")
LANES = 128


def exchange(blocks, axis):
    return lax.all_to_all(blocks, axis, 0, 0, tiled=True)


def copies(shard, axis):
    return exchange(jnp.broadcast_to(shard[None], (lax.axis_size(axis), *shard.shape)), axis)


def swap_cores(shard):
    return lax.ppermute(shard, "col", [(0, 1), (1, 0)])


def matmul(left, right):
    return jnp.dot(left, right, preferred_element_type=jnp.float32, precision=lax.Precision.HIGHEST)


def tmatmul(left, right):
    return lax.dot_general(
        left,
        right,
        (((0,), (0,)), ((), ())),
        preferred_element_type=jnp.float32,
        precision=lax.Precision.HIGHEST,
    )


def on_device(
    hamiltonian_rows, current_block, correction_block, previous_block, ritz_values, mixing_coeffs
):
    n_z, n_x, n_c = (lax.axis_size(a) for a in ("row_0", "row_1", "col"))
    width = current_block.shape[1]
    own_len = current_block.shape[0]
    out_rows = hamiltonian_rows.shape[2]
    window_total = out_rows * n_z * n_x * n_c
    core = lax.axis_index("col")

    direction = matmul(correction_block, mixing_coeffs[width : 2 * width]) + matmul(
        previous_block, mixing_coeffs[2 * width :]
    )
    mixed = matmul(current_block, mixing_coeffs[:width]) + direction
    next_block = mixed[:out_rows]
    next_direction = direction[:out_rows]

    own = jnp.concatenate([current_block, mixed], axis=1)
    other = swap_cores(own)
    tile = hamiltonian_rows.reshape(n_z, n_x, out_rows, n_c * own_len)
    tile = tile.transpose(1, 0, 2, 3).reshape(n_x * n_z * out_rows, n_c * own_len)
    own_tile = lax.dynamic_slice_in_dim(tile, core * own_len, own_len, 1)
    other_tile = lax.dynamic_slice_in_dim(tile, (1 - core) * own_len, own_len, 1)
    partial = matmul(own_tile, own) + matmul(other_tile, other)

    by_x = exchange(partial.reshape(n_x, n_z * out_rows, 2 * width), "row_1").sum(axis=0)
    lines = out_rows * 2 * width // LANES
    summed = exchange(by_x.reshape(n_z, lines, LANES), "row_0").sum(axis=0)
    summed = summed.reshape(out_rows, 2 * width)
    residual = summed[:, :width] - current_block[:out_rows] * ritz_values[None, :]
    squares = jnp.sum(residual * residual, axis=0)

    mine = jnp.concatenate(
        [
            summed[:, width:].reshape(-1, LANES),
            next_block.reshape(-1, LANES),
            squares.reshape(-1, LANES),
        ],
        axis=0,
    )
    n_lines = out_rows * width // LANES
    by_z = copies(mine, "row_0")
    square_z = by_z[:, 2 * n_lines :].sum(axis=0)
    rows_z = by_z[:, : 2 * n_lines].reshape(-1, LANES)
    gathered = copies(jnp.concatenate([rows_z, square_z], axis=0), "row_1")
    partner = swap_cores(gathered)

    def split(block):
        rows = block[:, : n_z * 2 * n_lines].reshape(n_x, n_z, 2, n_lines, LANES)
        product = rows[:, :, 0].reshape(-1, width)
        window = rows[:, :, 1].reshape(-1, width)
        grams = tmatmul(window, jnp.concatenate([product, window], axis=1))
        return grams, block[:, n_z * 2 * n_lines :].sum(axis=0)

    own_grams, own_squares = split(gathered)
    partner_grams, partner_squares = split(partner)
    grams = own_grams + partner_grams
    square_sum = (own_squares + partner_squares).reshape(width)
    next_correction = residual * lax.rsqrt(square_sum / window_total + 1e-06)
    return (next_block, next_direction, next_correction, grams[:, :width], grams[:, width:])


def solution(mesh):
    finer = Mesh(
        mesh.devices.reshape(mesh.shape["chan"], 16, 8, mesh.shape["col"]),
        ("chan", "row_0", "row_1", "col"),
    )
    in_specs = (
        P("chan", "col", None, ROW),
        P(CHAN_ROW_COL, None),
        P(CHAN_ROW_COL, None),
        P(CHAN_ROW_COL, None),
        P("chan"),
        P("chan", None),
    )
    out_specs = (
        P(CHAN_ROW_COL, None),
        P(CHAN_ROW_COL, None),
        P(CHAN_ROW_COL, None),
        P("chan", None),
        P("chan", None),
    )
    return jax.shard_map(
        on_device, mesh=finer, in_specs=in_specs, out_specs=out_specs, check_vma=False
    )
```

```python
import functools

import jax
import jax.numpy as jnp
from jax import lax
from jax.experimental import pallas as pl
from jax.experimental.pallas import tpu as pltpu
from jax.sharding import Mesh
from jax.sharding import PartitionSpec as P


ROW = ("row_0", "row_1")
CHAN_ROW_COL = ("chan", "row_0", "row_1", "col")
LANES = 128
SUBLANES = 8
MIB = 2**20
FILLER_FLOPS = 10**9
F32 = jnp.float32


def shape(*dims):
    return jax.ShapeDtypeStruct(dims, F32)


def exchange(blocks, axis):
    return lax.all_to_all(blocks, axis, 0, 0, tiled=True)


def swap_cores(shard):
    return lax.ppermute(shard, "col", [(0, 1), (1, 0)])


def matmul(left, right):
    return jnp.dot(left, right, preferred_element_type=F32, precision=lax.Precision.HIGHEST)


def call(kernel, out_shape, *args, in_spaces=None, scratch=(), flops=None, vmem=8):
    spaces = in_spaces or [pltpu.VMEM] * len(args)
    resident = pl.BlockSpec(memory_space=pltpu.VMEM)
    return pl.pallas_call(
        kernel,
        in_specs=[pl.BlockSpec(memory_space=space) for space in spaces],
        out_specs=jax.tree.map(lambda _: resident, out_shape),
        out_shape=out_shape,
        scratch_shapes=scratch,
        compiler_params=pltpu.CompilerParams(vmem_limit_bytes=vmem * MIB),
        cost_estimate=flops and pl.CostEstimate(flops=flops, transcendentals=0, bytes_accessed=0),
    )(*args)


def padded(count):
    return -(-count // SUBLANES) * SUBLANES


def partial_kernel(core, tile, other, part, own, ritz, out, scaled, block):
    n_x = out.shape[0]
    length = other.shape[0]
    per_x = part.shape[0] // n_x
    n_blocks = part.shape[1] // LANES
    n_rows, width = block.shape
    block[...] = own[:n_rows, width:]
    for b in range(width // LANES):
        at = slice(b * LANES, (b + 1) * LANES)
        scaled[b * n_rows : (b + 1) * n_rows] = own[:n_rows, at] * ritz[:, at]

    def finish(first):
        total = part[...] + matmul(tile[:, first : first + length], other[...])
        for i in range(n_x):
            for b in range(n_blocks):
                out[i, b * per_x : (b + 1) * per_x] = total[
                    i * per_x : (i + 1) * per_x, b * LANES : (b + 1) * LANES
                ]
            for b in range(width // LANES):
                first = n_blocks * per_x + b * n_rows
                lane = width + b * LANES
                out[i, first : first + n_rows] = own[:n_rows, lane : lane + LANES]
            last = n_blocks * per_x + n_rows * (width // LANES)
            if last < out.shape[1]:
                out[i, last:] = jnp.zeros((out.shape[1] - last, LANES), F32)

    @pl.when(core[0] == 0)
    def _():
        finish(length)

    @pl.when(core[0] != 0)
    def _():
        finish(0)


def sum_x_kernel(by_x, out, total, *, n_rows, n_blocks):
    n_x = by_x.shape[0]
    n_z = out.shape[0]
    per_block = n_z * n_rows
    n_sum = 2 * n_blocks * per_block
    running = by_x[0, :n_sum]
    for i in range(1, n_x):
        running = running + by_x[i, :n_sum]
    total[...] = running
    head = 2 * n_blocks * n_rows
    for b in range(n_blocks):
        for i in range(n_x):
            first = head + (b * n_x + i) * n_rows
            out[0, first : first + n_rows] = by_x[
                i, n_sum + b * n_rows : n_sum + (b + 1) * n_rows
            ]
    for z in range(n_z):
        if z:
            out[z, head:] = out[0, head:]
        for b in range(2 * n_blocks):
            first = b * per_block + z * n_rows
            out[z, b * n_rows : (b + 1) * n_rows] = total[first : first + n_rows]


def residual_kernel(by_z, scaled, residual, out, mine, *, n_rows, n_blocks):
    n_lines = n_blocks * n_rows
    running = by_z[0, : 2 * n_lines]
    for z in range(1, by_z.shape[0]):
        running = running + by_z[z, : 2 * n_lines]
    rest = running[:n_lines] - scaled[...]
    residual[...] = rest
    squares = rest * rest
    mine[...] = jnp.zeros(mine.shape, F32)
    mine[:n_lines] = running[n_lines:]
    for b in range(n_blocks):
        mine[n_lines + b : n_lines + b + 1] = jnp.sum(
            squares[b * n_rows : (b + 1) * n_rows], axis=0, keepdims=True
        )
    for z in range(out.shape[0]):
        out[z] = mine[...]


def window_kernel(by_z, window, *, n_x, n_rows, n_blocks):
    n_z = by_z.shape[0]
    head = 2 * n_blocks * n_rows
    for z in range(n_z):
        for b in range(n_blocks):
            for i in range(n_x):
                first = head + (b * n_x + i) * n_rows
                to = (i * n_z + z) * n_rows
                window[to : to + n_rows, b * LANES : (b + 1) * LANES] = by_z[
                    z, first : first + n_rows
                ]


def metric_kernel(own, other, own_t, other_t, metric):
    own_t[...] = own[...].T
    other_t[...] = other[...].T
    metric[...] = matmul(own_t[...], own[...]) + matmul(other_t[...], other[...])


def gather_kernel(by_z, out, *, n_rows, n_blocks):
    n_z = by_z.shape[0]
    n_lines = n_blocks * n_rows
    for z in range(n_z):
        for b in range(n_blocks):
            first = (b * n_z + z) * n_rows
            out[0, first : first + n_rows] = by_z[z, b * n_rows : (b + 1) * n_rows]
    running = by_z[0, n_lines : n_lines + n_blocks]
    for z in range(1, n_z):
        running = running + by_z[z, n_lines : n_lines + n_blocks]
    last = n_z * n_lines
    out[0, last:] = jnp.zeros((out.shape[1] - last, LANES), F32)
    out[0, last : last + n_blocks] = running
    for i in range(1, out.shape[0]):
        out[i] = out[0]


def matrix_of(lines, scratch, n_blocks, per_block):
    for i in range(lines.shape[0]):
        for b in range(n_blocks):
            scratch[i * per_block : (i + 1) * per_block, b * LANES : (b + 1) * LANES] = lines[
                i, b * per_block : (b + 1) * per_block
            ]


def square_of(lines, n_gathered, n_blocks):
    running = lines[0, n_gathered : n_gathered + n_blocks]
    for i in range(1, lines.shape[0]):
        running = running + lines[i, n_gathered : n_gathered + n_blocks]
    return running


def own_kernel(lines, window_t, ritz, scratch, *, n_blocks, per_block):
    matrix_of(lines, scratch, n_blocks, per_block)
    ritz[...] = matmul(window_t[...], scratch[...])


def final_kernel(
    part, lines, own_lines, window_t, residual, ritz, correction, scratch, *, n_blocks, per_block, total
):
    matrix_of(lines, scratch, n_blocks, per_block)
    ritz[...] = part[...] + matmul(window_t[...], scratch[...])
    n_rows = correction.shape[0]
    n_gathered = n_blocks * per_block
    squares = square_of(own_lines, n_gathered, n_blocks) + square_of(lines, n_gathered, n_blocks)
    scale = lax.rsqrt(squares / total + 1e-06)
    for b in range(n_blocks):
        correction[:, b * LANES : (b + 1) * LANES] = (
            residual[b * n_rows : (b + 1) * n_rows] * scale[b : b + 1]
        )


def step(
    hamiltonian_rows, current_block, correction_block, previous_block, ritz_values, mixing_coeffs
):
    n_z, n_x, n_c = (lax.axis_size(a) for a in ("row_0", "row_1", "col"))
    own_len, width = current_block.shape
    n_rows = hamiltonian_rows.shape[2]
    n_blocks = width // LANES
    window_total = n_rows * n_z * n_x * n_c
    per_block = n_z * n_rows
    n_lines = n_blocks * n_rows
    core = lax.axis_index("col")
    sizes = dict(n_rows=n_rows, n_blocks=n_blocks)

    direction = matmul(correction_block, mixing_coeffs[width : 2 * width]) + matmul(
        previous_block, mixing_coeffs[2 * width :]
    )
    mixed = matmul(current_block, mixing_coeffs[:width]) + direction
    own = jnp.concatenate([current_block, mixed], axis=1)
    next_direction = direction[:n_rows]

    other = swap_cores(own)
    tile = hamiltonian_rows.reshape(n_z, n_x, n_rows, n_c * own_len)
    tile = tile.transpose(1, 0, 2, 3).reshape(n_x * per_block, n_c * own_len)
    part = matmul(lax.dynamic_slice_in_dim(tile, core * own_len, own_len, 1), own)
    n_sum = 2 * n_blocks * per_block
    partial, scaled, next_block = call(
        partial_kernel,
        (
            shape(n_x, n_sum + padded(n_lines), LANES),
            shape(n_lines, LANES),
            shape(n_rows, width),
        ),
        core.reshape(1),
        tile,
        other,
        part,
        own,
        ritz_values[None],
        in_spaces=[pltpu.SMEM] + [pltpu.VMEM] * 5,
    )

    by_x = exchange(partial, "row_1")
    slots = call(
        functools.partial(sum_x_kernel, **sizes),
        shape(n_z, 2 * n_lines + n_x * n_lines, LANES),
        by_x,
        scratch=[pltpu.VMEM((n_sum, LANES), F32)],
    )
    by_z = exchange(slots, "row_0")
    residual, mine = call(
        functools.partial(residual_kernel, **sizes),
        (shape(n_lines, LANES), shape(n_z, padded(n_lines + n_blocks), LANES)),
        by_z,
        scaled,
        scratch=[pltpu.VMEM((padded(n_lines + n_blocks), LANES), F32)],
    )

    y_z = exchange(mine, "row_0")
    window = call(
        functools.partial(window_kernel, n_x=n_x, **sizes),
        shape(n_x * per_block, width),
        by_z,
        flops=FILLER_FLOPS,
    )
    own_t, other_t, metric_matrix = call(
        metric_kernel,
        (
            shape(width, n_x * per_block),
            shape(width, n_x * per_block),
            shape(width, width),
        ),
        window,
        swap_cores(window),
        flops=FILLER_FLOPS,
    )
    copies = call(
        functools.partial(gather_kernel, **sizes),
        shape(n_x, n_z * n_lines + padded(n_blocks), LANES),
        y_z,
    )
    y_x = exchange(copies, "row_1")
    other_y = swap_cores(y_x)
    scratch = [pltpu.VMEM((n_x * per_block, width), F32)]
    ritz_part = call(
        functools.partial(own_kernel, n_blocks=n_blocks, per_block=per_block),
        shape(width, width),
        y_x,
        own_t,
        scratch=scratch,
    )
    ritz_matrix, next_correction = call(
        functools.partial(
            final_kernel, n_blocks=n_blocks, per_block=per_block, total=window_total
        ),
        (shape(width, width), shape(n_rows, width)),
        ritz_part,
        other_y,
        y_x,
        other_t,
        residual,
        scratch=scratch,
    )
    return (next_block, next_direction, next_correction, ritz_matrix, metric_matrix)


def solution(mesh):
    finer = Mesh(
        mesh.devices.reshape(mesh.shape["chan"], 16, 8, mesh.shape["col"]),
        ("chan", "row_0", "row_1", "col"),
    )
    in_specs = (
        P("chan", "col", None, ROW),
        P(CHAN_ROW_COL, None),
        P(CHAN_ROW_COL, None),
        P(CHAN_ROW_COL, None),
        P("chan"),
        P("chan", None),
    )
    out_specs = (
        P(CHAN_ROW_COL, None),
        P(CHAN_ROW_COL, None),
        P(CHAN_ROW_COL, None),
        P("chan", None),
        P("chan", None),
    )
    return jax.shard_map(step, mesh=finer, in_specs=in_specs, out_specs=out_specs, check_vma=False)
```

```python
import functools

import jax
import jax.numpy as jnp
from jax import lax
from jax.experimental import pallas as pl
from jax.experimental.pallas import tpu as pltpu
from jax.sharding import Mesh
from jax.sharding import PartitionSpec as P

ROW = ("row_0", "row_1")
CHAN_ROW_COL = ("chan", "row_0", "row_1", "col")
LANES = 128
SUBLANES = 8
VMEM_BYTES = 8 * 2**20
F32 = jnp.float32


def shape(*dims):
    return jax.ShapeDtypeStruct(dims, F32)


def exchange(blocks, axis):
    return lax.all_to_all(blocks, axis, 0, 0, tiled=True)


def swap_cores(shard):
    return lax.ppermute(shard, "col", [(0, 1), (1, 0)])


def matmul(left, right):
    return jnp.dot(left, right, preferred_element_type=F32, precision=lax.Precision.HIGHEST)


def call(kernel, name, out_shape, *args, in_spaces=None, scratch=()):
    spaces = in_spaces or [pltpu.VMEM] * len(args)
    resident = pl.BlockSpec(memory_space=pltpu.VMEM)
    return pl.pallas_call(
        kernel,
        in_specs=[pl.BlockSpec(memory_space=space) for space in spaces],
        out_specs=jax.tree.map(lambda _: resident, out_shape),
        out_shape=out_shape,
        scratch_shapes=scratch,
        compiler_params=pltpu.CompilerParams(vmem_limit_bytes=VMEM_BYTES),
        name=name,
    )(*args)


def padded(count):
    return -(-count // SUBLANES) * SUBLANES


def partial_kernel(core, tile, other, part, scaled, direction, out, scaled_lines, first_rows):
    n_x = out.shape[0]
    length = other.shape[0]
    per_x = part.shape[0] // n_x
    n_blocks = part.shape[1] // LANES
    n_rows, width = first_rows.shape
    first_rows[...] = direction[:n_rows]
    for b in range(width // LANES):
        at = slice(b * LANES, (b + 1) * LANES)
        scaled_lines[b * n_rows : (b + 1) * n_rows] = scaled[:, at]

    def finish(first):
        total = part[...] + matmul(tile[:, first : first + length], other[...])
        for i in range(n_x):
            for b in range(n_blocks):
                out[i, b * per_x : (b + 1) * per_x] = total[
                    i * per_x : (i + 1) * per_x, b * LANES : (b + 1) * LANES
                ]

    @pl.when(core[0] == 0)
    def _():
        finish(length)

    @pl.when(core[0] != 0)
    def _():
        finish(0)


def sum_x_kernel(by_x, own, out, block, lines, total, *, n_rows, n_blocks):
    n_x = by_x.shape[0]
    n_z = out.shape[0]
    running = by_x[0]
    for i in range(1, n_x):
        running = running + by_x[i]
    total[...] = running
    for z in range(n_z):
        for b in range(2 * n_blocks):
            first = (b * n_z + z) * n_rows
            out[z, b * n_rows : (b + 1) * n_rows] = total[first : first + n_rows]
    first = n_blocks * LANES
    block[...] = own[:n_rows, first:]
    for b in range(n_blocks):
        at = slice(first + b * LANES, first + (b + 1) * LANES)
        lines[b * n_rows : (b + 1) * n_rows] = own[:n_rows, at]


def residual_kernel(by_z, scaled, lines, residual, out, mine, *, n_rows, n_blocks):
    n_lines = n_blocks * n_rows
    running = by_z[0]
    for z in range(1, by_z.shape[0]):
        running = running + by_z[z]
    rest = running[:n_lines] - scaled[...]
    residual[...] = rest
    squares = rest * rest
    mine[...] = jnp.zeros(mine.shape, F32)
    mine[:n_lines] = running[n_lines:]
    mine[n_lines : 2 * n_lines] = lines[...]
    for b in range(n_blocks):
        at = slice(b * n_rows, (b + 1) * n_rows)
        mine[2 * n_lines + b : 2 * n_lines + b + 1] = jnp.sum(squares[at], axis=0, keepdims=True)
    for z in range(out.shape[0]):
        out[z] = mine[...]


def gather_kernel(by_z, out, *, n_rows, n_blocks):
    n_z = by_z.shape[0]
    n_lines = 2 * n_blocks * n_rows
    for z in range(n_z):
        for b in range(2 * n_blocks):
            first = (b * n_z + z) * n_rows
            out[0, first : first + n_rows] = by_z[z, b * n_rows : (b + 1) * n_rows]
    running = by_z[0, n_lines : n_lines + n_blocks]
    for z in range(1, n_z):
        running = running + by_z[z, n_lines : n_lines + n_blocks]
    last = n_z * n_lines
    out[0, last:] = jnp.zeros((out.shape[1] - last, LANES), F32)
    out[0, last : last + n_blocks] = running
    for i in range(1, out.shape[0]):
        out[i] = out[0]


def grams(lines, product, window, n_blocks, per_block):
    for i in range(lines.shape[0]):
        to = slice(i * per_block, (i + 1) * per_block)
        for b in range(n_blocks):
            at = slice(b * LANES, (b + 1) * LANES)
            product[to, at] = lines[i, b * per_block : (b + 1) * per_block]
            first = (n_blocks + b) * per_block
            window[to, at] = lines[i, first : first + per_block]
    turned = window[...].T
    return matmul(turned, product[...]), matmul(turned, window[...])


def square_of(lines, n_gathered, n_blocks):
    running = lines[0, n_gathered : n_gathered + n_blocks]
    for i in range(1, lines.shape[0]):
        running = running + lines[i, n_gathered : n_gathered + n_blocks]
    return running


def own_kernel(lines, ritz, metric, product, window, *, n_blocks, per_block):
    ritz[...], metric[...] = grams(lines, product, window, n_blocks, per_block)


def final_kernel(
    ritz_part, metric_part, lines, own_lines, residual, ritz, metric, correction, product, window,
    *, n_blocks, per_block, total
):
    other_ritz, other_metric = grams(lines, product, window, n_blocks, per_block)
    ritz[...] = ritz_part[...] + other_ritz
    metric[...] = metric_part[...] + other_metric
    n_rows = correction.shape[0]
    n_gathered = 2 * n_blocks * per_block
    squares = square_of(own_lines, n_gathered, n_blocks) + square_of(lines, n_gathered, n_blocks)
    scale = lax.rsqrt(squares / total + 1e-06)
    for b in range(n_blocks):
        correction[:, b * LANES : (b + 1) * LANES] = (
            residual[b * n_rows : (b + 1) * n_rows] * scale[b : b + 1]
        )


def on_device(
    hamiltonian_rows, current_block, correction_block, previous_block, ritz_values, mixing_coeffs
):
    n_z, n_x, n_c = (lax.axis_size(a) for a in ("row_0", "row_1", "col"))
    own_len, width = current_block.shape
    n_rows = hamiltonian_rows.shape[2]
    n_blocks = width // LANES
    window_total = n_rows * n_z * n_x * n_c
    per_block = n_z * n_rows
    n_lines = n_blocks * n_rows
    core = lax.axis_index("col")
    sizes = dict(n_rows=n_rows, n_blocks=n_blocks)

    direction = matmul(correction_block, mixing_coeffs[width : 2 * width]) + matmul(
        previous_block, mixing_coeffs[2 * width :]
    )
    mixed = matmul(current_block, mixing_coeffs[:width]) + direction
    own = jnp.concatenate([current_block, mixed], axis=1)
    scaled_rows = current_block[:n_rows] * ritz_values[None, :]

    other = swap_cores(own)
    tile = hamiltonian_rows.reshape(n_z, n_x, n_rows, n_c * own_len)
    tile = tile.transpose(1, 0, 2, 3).reshape(n_x * per_block, n_c * own_len)
    part = matmul(lax.dynamic_slice_in_dim(tile, core * own_len, own_len, 1), own)
    n_sum = 2 * n_blocks * per_block
    partial, scaled, next_direction = call(
        partial_kernel,
        "partial",
        (shape(n_x, n_sum, LANES), shape(n_lines, LANES), shape(n_rows, width)),
        core.reshape(1),
        tile,
        other,
        part,
        scaled_rows,
        direction,
        in_spaces=[pltpu.SMEM] + [pltpu.VMEM] * 5,
    )

    by_x = exchange(partial, "row_1")
    slots, next_block, block_lines = call(
        functools.partial(sum_x_kernel, **sizes),
        "sum_x",
        (shape(n_z, 2 * n_lines, LANES), shape(n_rows, width), shape(n_lines, LANES)),
        by_x,
        own,
        scratch=[pltpu.VMEM((n_sum, LANES), F32)],
    )
    by_z = exchange(slots, "row_0")
    n_mine = padded(2 * n_lines + n_blocks)
    residual, mine = call(
        functools.partial(residual_kernel, **sizes),
        "residual",
        (shape(n_lines, LANES), shape(n_z, n_mine, LANES)),
        by_z,
        scaled,
        block_lines,
        scratch=[pltpu.VMEM((n_mine, LANES), F32)],
    )

    copies = call(
        functools.partial(gather_kernel, **sizes),
        "gather",
        shape(n_x, 2 * n_z * n_lines + padded(n_blocks), LANES),
        exchange(mine, "row_0"),
    )
    lines = exchange(copies, "row_1")
    other_lines = swap_cores(lines)
    scratch = [pltpu.VMEM((n_x * per_block, width), F32)] * 2
    ritz_part, metric_part = call(
        functools.partial(own_kernel, n_blocks=n_blocks, per_block=per_block),
        "own_grams",
        (shape(width, width), shape(width, width)),
        lines,
        scratch=scratch,
    )
    ritz_matrix, metric_matrix, next_correction = call(
        functools.partial(
            final_kernel, n_blocks=n_blocks, per_block=per_block, total=window_total
        ),
        "final",
        (shape(width, width), shape(width, width), shape(n_rows, width)),
        ritz_part,
        metric_part,
        other_lines,
        lines,
        residual,
        scratch=scratch,
    )
    return (next_block, next_direction, next_correction, ritz_matrix, metric_matrix)


def solution(mesh):
    finer = Mesh(
        mesh.devices.reshape(mesh.shape["chan"], 16, 8, mesh.shape["col"]),
        ("chan", "row_0", "row_1", "col"),
    )
    in_specs = (
        P("chan", "col", None, ROW),
        P(CHAN_ROW_COL, None),
        P(CHAN_ROW_COL, None),
        P(CHAN_ROW_COL, None),
        P("chan"),
        P("chan", None),
    )
    out_specs = (
        P(CHAN_ROW_COL, None),
        P(CHAN_ROW_COL, None),
        P(CHAN_ROW_COL, None),
        P("chan", None),
        P("chan", None),
    )
    return jax.shard_map(
        on_device, mesh=finer, in_specs=in_specs, out_specs=out_specs, check_vma=False
    )
```

```python
import functools

import jax
import jax.numpy as jnp
from jax import lax
from jax.experimental import pallas as pl
from jax.experimental.pallas import tpu as pltpu
from jax.sharding import Mesh
from jax.sharding import PartitionSpec as P

ROW = ("row_0", "row_1")
CHAN_ROW_COL = ("chan", "row_0", "row_1", "col")
LANES = 128
SUBLANES = 8
VMEM_BYTES = 8 * 2**20
F32 = jnp.float32


def shape(*dims):
    return jax.ShapeDtypeStruct(dims, F32)


def exchange(blocks, axis):
    return lax.all_to_all(blocks, axis, 0, 0, tiled=True)


def swap_cores(shard):
    return lax.ppermute(shard, "col", [(0, 1), (1, 0)])


def matmul(left, right):
    return jnp.dot(left, right, preferred_element_type=F32, precision=lax.Precision.HIGHEST)


def call(kernel, name, out_shape, *args, in_spaces=None, scratch=()):
    spaces = in_spaces or [pltpu.VMEM] * len(args)
    resident = pl.BlockSpec(memory_space=pltpu.VMEM)
    return pl.pallas_call(
        kernel,
        in_specs=[pl.BlockSpec(memory_space=space) for space in spaces],
        out_specs=jax.tree.map(lambda _: resident, out_shape),
        out_shape=out_shape,
        scratch_shapes=scratch,
        compiler_params=pltpu.CompilerParams(vmem_limit_bytes=VMEM_BYTES),
        name=name,
    )(*args)


def padded(count):
    return -(-count // SUBLANES) * SUBLANES


def partial_kernel(
    core, tile, other_x, other_b, part_x, part_b, scaled, mixed, out, scaled_lines, block_lines
):
    n_x = out.shape[0]
    n_rows, width = scaled.shape
    length = other_x.shape[0]
    per_x = part_x.shape[0] // n_x
    n_blocks = width // LANES
    for b in range(n_blocks):
        at = slice(b * LANES, (b + 1) * LANES)
        scaled_lines[b * n_rows : (b + 1) * n_rows] = scaled[:, at]
        block_lines[b * n_rows : (b + 1) * n_rows] = mixed[:n_rows, at]

    def finish(first):
        for half, (part, other) in enumerate(((part_x, other_x), (part_b, other_b))):
            total = part[...] + matmul(tile[:, first : first + length], other[...])
            for i in range(n_x):
                for b in range(n_blocks):
                    to = (half * n_blocks + b) * per_x
                    out[i, to : to + per_x] = total[
                        i * per_x : (i + 1) * per_x, b * LANES : (b + 1) * LANES
                    ]

    @pl.when(core[0] == 0)
    def _():
        finish(length)

    @pl.when(core[0] != 0)
    def _():
        finish(0)


def sum_x_kernel(by_x, out, total, *, n_rows, n_blocks):
    n_x = by_x.shape[0]
    n_z = out.shape[0]
    running = by_x[0]
    for i in range(1, n_x):
        running = running + by_x[i]
    total[...] = running
    for z in range(n_z):
        for b in range(2 * n_blocks):
            first = (b * n_z + z) * n_rows
            out[z, b * n_rows : (b + 1) * n_rows] = total[first : first + n_rows]


def residual_kernel(by_z, scaled, lines, residual, out, *, n_rows, n_blocks):
    n_lines = n_blocks * n_rows
    running = by_z[0]
    for z in range(1, by_z.shape[0]):
        running = running + by_z[z]
    rest = running[:n_lines] - scaled[...]
    residual[...] = rest
    squares = rest * rest
    out[0, 0] = running[n_lines:]
    out[0, 1] = lines[...]
    out[0, 2] = jnp.zeros((n_lines, LANES), F32)
    for b in range(n_blocks):
        at = slice(b * n_rows, (b + 1) * n_rows)
        out[0, 2, b : b + 1] = jnp.sum(squares[at], axis=0, keepdims=True)
    for z in range(1, out.shape[0]):
        out[z] = out[0]


def gather_kernel(by_z, out, *, n_rows, n_blocks):
    n_z = by_z.shape[0]
    n_lines = n_blocks * n_rows
    for z in range(n_z):
        for part in range(2):
            for b in range(n_blocks):
                first = ((part * n_blocks + b) * n_z + z) * n_rows
                out[0, first : first + n_rows] = by_z[z, part, b * n_rows : (b + 1) * n_rows]
    running = by_z[0, 2]
    for z in range(1, n_z):
        running = running + by_z[z, 2]
    last = 2 * n_z * n_lines
    out[0, last:] = jnp.zeros((out.shape[1] - last, LANES), F32)
    out[0, last : last + n_blocks] = running[:n_blocks]
    for i in range(1, out.shape[0]):
        out[i] = out[0]


def grams(lines, product, window, n_blocks, per_block):
    for i in range(lines.shape[0]):
        to = slice(i * per_block, (i + 1) * per_block)
        for b in range(n_blocks):
            at = slice(b * LANES, (b + 1) * LANES)
            product[to, at] = lines[i, b * per_block : (b + 1) * per_block]
            first = (n_blocks + b) * per_block
            window[to, at] = lines[i, first : first + per_block]
    turned = window[...].T
    return matmul(turned, product[...]), matmul(turned, window[...])


def square_of(lines, n_gathered, n_blocks):
    running = lines[0, n_gathered : n_gathered + n_blocks]
    for i in range(1, lines.shape[0]):
        running = running + lines[i, n_gathered : n_gathered + n_blocks]
    return running


def own_kernel(
    lines, mixed, direction, ritz, metric, block, first_rows, product, window, *, n_blocks, per_block
):
    block[...] = mixed[: block.shape[0]]
    first_rows[...] = direction[: block.shape[0]]
    ritz[...], metric[...] = grams(lines, product, window, n_blocks, per_block)


def final_kernel(
    ritz_part, metric_part, lines, own_lines, residual, ritz, metric, correction, product, window,
    *, n_blocks, per_block, total
):
    other_ritz, other_metric = grams(lines, product, window, n_blocks, per_block)
    ritz[...] = ritz_part[...] + other_ritz
    metric[...] = metric_part[...] + other_metric
    n_rows = correction.shape[0]
    n_gathered = 2 * n_blocks * per_block
    squares = square_of(own_lines, n_gathered, n_blocks) + square_of(lines, n_gathered, n_blocks)
    scale = lax.rsqrt(squares / total + 1e-06)
    for b in range(n_blocks):
        correction[:, b * LANES : (b + 1) * LANES] = (
            residual[b * n_rows : (b + 1) * n_rows] * scale[b : b + 1]
        )


def on_device(
    hamiltonian_rows, current_block, correction_block, previous_block, ritz_values, mixing_coeffs
):
    n_z, n_x, n_c = (lax.axis_size(a) for a in ("row_0", "row_1", "col"))
    own_len, width = current_block.shape
    n_rows = hamiltonian_rows.shape[2]
    n_blocks = width // LANES
    window_total = n_rows * n_z * n_x * n_c
    per_block = n_z * n_rows
    n_lines = n_blocks * n_rows
    core = lax.axis_index("col")
    sizes = dict(n_rows=n_rows, n_blocks=n_blocks)

    other_x = swap_cores(current_block)
    direction = matmul(correction_block, mixing_coeffs[width : 2 * width]) + matmul(
        previous_block, mixing_coeffs[2 * width :]
    )
    mixed = matmul(current_block, mixing_coeffs[:width]) + direction
    other_b = swap_cores(mixed)
    scaled_rows = current_block[:n_rows] * ritz_values[None, :]

    tile = hamiltonian_rows.reshape(n_z, n_x, n_rows, n_c * own_len)
    tile = tile.transpose(1, 0, 2, 3).reshape(n_x * per_block, n_c * own_len)
    own_tile = lax.dynamic_slice_in_dim(tile, core * own_len, own_len, 1)
    n_sum = 2 * n_blocks * per_block
    partial, scaled, block_lines = call(
        partial_kernel,
        "partial",
        (shape(n_x, n_sum, LANES), shape(n_lines, LANES), shape(n_lines, LANES)),
        core.reshape(1),
        tile,
        other_x,
        other_b,
        matmul(own_tile, current_block),
        matmul(own_tile, mixed),
        scaled_rows,
        mixed,
        in_spaces=[pltpu.SMEM] + [pltpu.VMEM] * 7,
    )

    by_x = exchange(partial, "row_1")
    slots = call(
        functools.partial(sum_x_kernel, **sizes),
        "sum_x",
        shape(n_z, 2 * n_lines, LANES),
        by_x,
        scratch=[pltpu.VMEM((n_sum, LANES), F32)],
    )
    by_z = exchange(slots, "row_0")
    residual, mine = call(
        functools.partial(residual_kernel, **sizes),
        "residual",
        (shape(n_lines, LANES), shape(n_z, 3, n_lines, LANES)),
        by_z,
        scaled,
        block_lines,
    )

    copies = call(
        functools.partial(gather_kernel, **sizes),
        "gather",
        shape(n_x, 2 * n_z * n_lines + padded(n_blocks), LANES),
        exchange(mine, "row_0"),
    )
    lines = exchange(copies, "row_1")
    other_lines = swap_cores(lines)
    scratch = [pltpu.VMEM((n_x * per_block, width), F32)] * 2
    ritz_part, metric_part, next_block, next_direction = call(
        functools.partial(own_kernel, n_blocks=n_blocks, per_block=per_block),
        "own_grams",
        (shape(width, width), shape(width, width), shape(n_rows, width), shape(n_rows, width)),
        lines,
        mixed,
        direction,
        scratch=scratch,
    )
    ritz_matrix, metric_matrix, next_correction = call(
        functools.partial(
            final_kernel, n_blocks=n_blocks, per_block=per_block, total=window_total
        ),
        "final",
        (shape(width, width), shape(width, width), shape(n_rows, width)),
        ritz_part,
        metric_part,
        other_lines,
        lines,
        residual,
        scratch=scratch,
    )
    return (next_block, next_direction, next_correction, ritz_matrix, metric_matrix)


def solution(mesh):
    finer = Mesh(
        mesh.devices.reshape(mesh.shape["chan"], 16, 8, mesh.shape["col"]),
        ("chan", "row_0", "row_1", "col"),
    )
    in_specs = (
        P("chan", "col", None, ROW),
        P(CHAN_ROW_COL, None),
        P(CHAN_ROW_COL, None),
        P(CHAN_ROW_COL, None),
        P("chan"),
        P("chan", None),
    )
    out_specs = (
        P(CHAN_ROW_COL, None),
        P(CHAN_ROW_COL, None),
        P(CHAN_ROW_COL, None),
        P("chan", None),
        P("chan", None),
    )
    return jax.shard_map(
        on_device, mesh=finer, in_specs=in_specs, out_specs=out_specs, check_vma=False
    )
```

```python
import functools

import jax
import jax.numpy as jnp
from jax import lax
from jax.experimental import pallas as pl
from jax.experimental.pallas import tpu as pltpu
from jax.sharding import Mesh
from jax.sharding import PartitionSpec as P

ROW = ("row_0", "row_1")
CHAN_ROW_COL = ("chan", "row_0", "row_1", "col")
LANES = 128
SUBLANES = 8
VMEM_BYTES = 8 * 2**20
F32 = jnp.float32


def shape(*dims):
    return jax.ShapeDtypeStruct(dims, F32)


def exchange(blocks, axis):
    return lax.all_to_all(blocks, axis, 0, 0, tiled=True)


def swap_cores(shard):
    return lax.ppermute(shard, "col", [(0, 1), (1, 0)])


def matmul(left, right):
    return jnp.dot(left, right, preferred_element_type=F32, precision=lax.Precision.HIGHEST)


def call(kernel, name, out_shape, *args, in_spaces=None, scratch=()):
    spaces = in_spaces or [pltpu.VMEM] * len(args)
    resident = pl.BlockSpec(memory_space=pltpu.VMEM)
    return pl.pallas_call(
        kernel,
        in_specs=[pl.BlockSpec(memory_space=space) for space in spaces],
        out_specs=jax.tree.map(lambda _: resident, out_shape),
        out_shape=out_shape,
        scratch_shapes=scratch,
        compiler_params=pltpu.CompilerParams(vmem_limit_bytes=VMEM_BYTES),
        name=name,
    )(*args)


def padded(count):
    return -(-count // SUBLANES) * SUBLANES


def partial_kernel(
    core, tile, other, part, scaled, own, out, scaled_lines, block_lines
):
    n_x = out.shape[0]
    n_rows, width = scaled.shape
    length = other.shape[0]
    per_x = part.shape[0] // n_x
    n_blocks = width // LANES
    for b in range(n_blocks):
        at = slice(b * LANES, (b + 1) * LANES)
        scaled_lines[b * n_rows : (b + 1) * n_rows] = scaled[:, at]
        block_lines[b * n_rows : (b + 1) * n_rows] = own[
            :n_rows, width + b * LANES : width + (b + 1) * LANES
        ]

    def finish(first):
        total = part[...] + matmul(tile[:, first : first + length], other[...])
        for i in range(n_x):
            for b in range(2 * n_blocks):
                out[i, b * per_x : (b + 1) * per_x] = total[
                    i * per_x : (i + 1) * per_x, b * LANES : (b + 1) * LANES
                ]

    @pl.when(core[0] == 0)
    def _():
        finish(length)

    @pl.when(core[0] != 0)
    def _():
        finish(0)


def sum_x_kernel(by_x, out, total, *, n_rows, n_blocks):
    n_x = by_x.shape[0]
    n_z = out.shape[0]
    running = by_x[0]
    for i in range(1, n_x):
        running = running + by_x[i]
    total[...] = running
    for z in range(n_z):
        for b in range(2 * n_blocks):
            first = (b * n_z + z) * n_rows
            out[z, b * n_rows : (b + 1) * n_rows] = total[first : first + n_rows]


def residual_kernel(by_z, scaled, lines, residual, out, *, n_rows, n_blocks):
    n_lines = n_blocks * n_rows
    running = by_z[0]
    for z in range(1, by_z.shape[0]):
        running = running + by_z[z]
    rest = running[:n_lines] - scaled[...]
    residual[...] = rest
    squares = rest * rest
    out[0, 0] = running[n_lines:]
    out[0, 1] = lines[...]
    out[0, 2] = jnp.zeros((n_lines, LANES), F32)
    for b in range(n_blocks):
        at = slice(b * n_rows, (b + 1) * n_rows)
        out[0, 2, b : b + 1] = jnp.sum(squares[at], axis=0, keepdims=True)
    for z in range(1, out.shape[0]):
        out[z] = out[0]


def gather_kernel(by_z, out, *, n_rows, n_blocks):
    n_z = by_z.shape[0]
    n_lines = n_blocks * n_rows
    for z in range(n_z):
        for part in range(2):
            for b in range(n_blocks):
                first = ((part * n_blocks + b) * n_z + z) * n_rows
                out[0, first : first + n_rows] = by_z[z, part, b * n_rows : (b + 1) * n_rows]
    running = by_z[0, 2]
    for z in range(1, n_z):
        running = running + by_z[z, 2]
    last = 2 * n_z * n_lines
    out[0, last:] = jnp.zeros((out.shape[1] - last, LANES), F32)
    out[0, last : last + n_blocks] = running[:n_blocks]
    for i in range(1, out.shape[0]):
        out[i] = out[0]


def own_kernel(lines, packed, product, window, *, n_blocks, per_block):
    n_x = lines.shape[0]
    width = product.shape[1]
    for i in range(n_x):
        to = slice(i * per_block, (i + 1) * per_block)
        for b in range(n_blocks):
            at = slice(b * LANES, (b + 1) * LANES)
            product[to, at] = lines[i, b * per_block : (b + 1) * per_block]
            first = (n_blocks + b) * per_block
            window[to, at] = lines[i, first : first + per_block]
    turned = window[...].T
    packed[:width, :width] = matmul(turned, product[...])
    packed[:width, width:] = matmul(turned, window[...])
    last = 2 * n_blocks * per_block
    running = lines[0, last:]
    for i in range(1, n_x):
        running = running + lines[i, last:]
    packed[width:] = jnp.zeros((packed.shape[0] - width, 2 * width), F32)
    for b in range(n_blocks):
        packed[width : width + 1, b * LANES : (b + 1) * LANES] = running[b : b + 1]


def final_kernel(
    mine, other, residual, own, direction, block, first_rows, correction, ritz, metric, *, total
):
    n_rows, width = block.shape
    block[...] = own[:n_rows, width:]
    first_rows[...] = direction[:n_rows]
    ritz[...] = mine[:width, :width] + other[:width, :width]
    metric[...] = mine[:width, width:] + other[:width, width:]
    squares = mine[width : width + 1, :width] + other[width : width + 1, :width]
    scale = lax.rsqrt(squares / total + 1e-06)
    for b in range(width // LANES):
        at = slice(b * LANES, (b + 1) * LANES)
        correction[:, at] = residual[b * n_rows : (b + 1) * n_rows] * scale[:, at]


def on_device(
    hamiltonian_rows, current_block, correction_block, previous_block, ritz_values, mixing_coeffs
):
    n_z, n_x, n_c = (lax.axis_size(a) for a in ("row_0", "row_1", "col"))
    own_len, width = current_block.shape
    n_rows = hamiltonian_rows.shape[2]
    n_blocks = width // LANES
    window_total = n_rows * n_z * n_x * n_c
    per_block = n_z * n_rows
    n_lines = n_blocks * n_rows
    core = lax.axis_index("col")
    sizes = dict(n_rows=n_rows, n_blocks=n_blocks)

    direction = matmul(correction_block, mixing_coeffs[width : 2 * width]) + matmul(
        previous_block, mixing_coeffs[2 * width :]
    )
    mixed = matmul(current_block, mixing_coeffs[:width]) + direction
    own = jnp.concatenate([current_block, mixed], axis=1)
    other = swap_cores(own)
    scaled_rows = current_block[:n_rows] * ritz_values[None, :]

    tile = hamiltonian_rows.reshape(n_z, n_x, n_rows, n_c * own_len)
    tile = tile.transpose(1, 0, 2, 3).reshape(n_x * per_block, n_c * own_len)
    own_tile = lax.dynamic_slice_in_dim(tile, core * own_len, own_len, 1)
    n_sum = 2 * n_blocks * per_block
    partial, scaled, block_lines = call(
        partial_kernel,
        "partial",
        (shape(n_x, n_sum, LANES), shape(n_lines, LANES), shape(n_lines, LANES)),
        core.reshape(1),
        tile,
        other,
        matmul(own_tile, own),
        scaled_rows,
        own,
        in_spaces=[pltpu.SMEM] + [pltpu.VMEM] * 5,
    )

    by_x = exchange(partial, "row_1")
    slots = call(
        functools.partial(sum_x_kernel, **sizes),
        "sum_x",
        shape(n_z, 2 * n_lines, LANES),
        by_x,
        scratch=[pltpu.VMEM((n_sum, LANES), F32)],
    )
    by_z = exchange(slots, "row_0")
    residual, mine = call(
        functools.partial(residual_kernel, **sizes),
        "residual",
        (shape(n_lines, LANES), shape(n_z, 3, n_lines, LANES)),
        by_z,
        scaled,
        block_lines,
    )

    copies = call(
        functools.partial(gather_kernel, **sizes),
        "gather",
        shape(n_x, 2 * n_z * n_lines + padded(n_blocks), LANES),
        exchange(mine, "row_0"),
    )
    lines = exchange(copies, "row_1")
    packed = call(
        functools.partial(own_kernel, n_blocks=n_blocks, per_block=per_block),
        "own_grams",
        shape(width + SUBLANES, 2 * width),
        lines,
        scratch=[pltpu.VMEM((n_x * per_block, width), F32)] * 2,
    )
    return call(
        functools.partial(final_kernel, total=window_total),
        "final",
        (shape(n_rows, width),) * 3 + (shape(width, width),) * 2,
        packed,
        swap_cores(packed),
        residual,
        own,
        direction,
    )


def solution(mesh):
    finer = Mesh(
        mesh.devices.reshape(mesh.shape["chan"], 16, 8, mesh.shape["col"]),
        ("chan", "row_0", "row_1", "col"),
    )
    in_specs = (
        P("chan", "col", None, ROW),
        P(CHAN_ROW_COL, None),
        P(CHAN_ROW_COL, None),
        P(CHAN_ROW_COL, None),
        P("chan"),
        P("chan", None),
    )
    out_specs = (
        P(CHAN_ROW_COL, None),
        P(CHAN_ROW_COL, None),
        P(CHAN_ROW_COL, None),
        P("chan", None),
        P("chan", None),
    )
    return jax.shard_map(
        on_device, mesh=finer, in_specs=in_specs, out_specs=out_specs, check_vma=False
    )
```

```python
import functools

import jax
import jax.numpy as jnp
from jax import lax
from jax.experimental import pallas as pl
from jax.experimental.pallas import tpu as pltpu
from jax.sharding import Mesh
from jax.sharding import PartitionSpec as P

ROW = ("row_0", "row_1")
CHAN_ROW_COL = ("chan", "row_0", "row_1", "col")
LANES = 128
SUBLANES = 8
VMEM_BYTES = 8 * 2**20
F32 = jnp.float32


def shape(*dims):
    return jax.ShapeDtypeStruct(dims, F32)


def exchange(blocks, axis):
    return lax.all_to_all(blocks, axis, 0, 0, tiled=True)


def swap_cores(shard):
    return lax.ppermute(shard, "col", [(0, 1), (1, 0)])


def matmul(left, right):
    return jnp.dot(left, right, preferred_element_type=F32, precision=lax.Precision.HIGHEST)


def call(kernel, name, out_shape, *args, in_spaces=None, scratch=()):
    spaces = in_spaces or [pltpu.VMEM] * len(args)
    resident = pl.BlockSpec(memory_space=pltpu.VMEM)
    return pl.pallas_call(
        kernel,
        in_specs=[pl.BlockSpec(memory_space=space) for space in spaces],
        out_specs=jax.tree.map(lambda _: resident, out_shape),
        out_shape=out_shape,
        scratch_shapes=scratch,
        compiler_params=pltpu.CompilerParams(vmem_limit_bytes=VMEM_BYTES),
        name=name,
    )(*args)


def padded(count):
    return -(-count // SUBLANES) * SUBLANES


def mix_kernel(x, w, p, c, own, direction):
    width = x.shape[1]
    total = matmul(w[...], c[width : 2 * width]) + matmul(p[...], c[2 * width :])
    direction[...] = total[: direction.shape[0]]
    own[:, :width] = x[...]
    own[:, width:] = total + matmul(x[...], c[:width])


def partial_kernel(
    core, tile, other, part, scaled, own, out, scaled_lines, block_lines
):
    n_x = out.shape[0]
    n_rows, width = scaled.shape
    length = other.shape[0]
    per_x = part.shape[0] // n_x
    n_blocks = width // LANES
    for b in range(n_blocks):
        at = slice(b * LANES, (b + 1) * LANES)
        scaled_lines[b * n_rows : (b + 1) * n_rows] = scaled[:, at]
        block_lines[b * n_rows : (b + 1) * n_rows] = own[
            :n_rows, width + b * LANES : width + (b + 1) * LANES
        ]

    def finish(first):
        total = part[...] + matmul(tile[:, first : first + length], other[...])
        for i in range(n_x):
            for b in range(2 * n_blocks):
                out[i, b * per_x : (b + 1) * per_x] = total[
                    i * per_x : (i + 1) * per_x, b * LANES : (b + 1) * LANES
                ]

    @pl.when(core[0] == 0)
    def _():
        finish(length)

    @pl.when(core[0] != 0)
    def _():
        finish(0)


def sum_x_kernel(by_x, out, total, *, n_rows, n_blocks):
    n_x = by_x.shape[0]
    n_z = out.shape[0]
    running = by_x[0]
    for i in range(1, n_x):
        running = running + by_x[i]
    total[...] = running
    for z in range(n_z):
        for b in range(2 * n_blocks):
            first = (b * n_z + z) * n_rows
            out[z, b * n_rows : (b + 1) * n_rows] = total[first : first + n_rows]


def residual_kernel(by_z, scaled, lines, residual, out, *, n_rows, n_blocks):
    n_lines = n_blocks * n_rows
    running = by_z[0]
    for z in range(1, by_z.shape[0]):
        running = running + by_z[z]
    rest = running[:n_lines] - scaled[...]
    residual[...] = rest
    squares = rest * rest
    out[0, 0] = running[n_lines:]
    out[0, 1] = lines[...]
    out[0, 2] = jnp.zeros((n_lines, LANES), F32)
    for b in range(n_blocks):
        at = slice(b * n_rows, (b + 1) * n_rows)
        out[0, 2, b : b + 1] = jnp.sum(squares[at], axis=0, keepdims=True)
    for z in range(1, out.shape[0]):
        out[z] = out[0]


def gather_kernel(by_z, out, *, n_rows, n_blocks):
    n_z = by_z.shape[0]
    n_lines = n_blocks * n_rows
    for z in range(n_z):
        for part in range(2):
            for b in range(n_blocks):
                first = ((part * n_blocks + b) * n_z + z) * n_rows
                out[0, first : first + n_rows] = by_z[z, part, b * n_rows : (b + 1) * n_rows]
    running = by_z[0, 2]
    for z in range(1, n_z):
        running = running + by_z[z, 2]
    last = 2 * n_z * n_lines
    out[0, last:] = jnp.zeros((out.shape[1] - last, LANES), F32)
    out[0, last : last + n_blocks] = running[:n_blocks]
    for i in range(1, out.shape[0]):
        out[i] = out[0]


def own_kernel(lines, packed, product, window, *, n_blocks, per_block):
    n_x = lines.shape[0]
    width = product.shape[1]
    for i in range(n_x):
        to = slice(i * per_block, (i + 1) * per_block)
        for b in range(n_blocks):
            at = slice(b * LANES, (b + 1) * LANES)
            product[to, at] = lines[i, b * per_block : (b + 1) * per_block]
            first = (n_blocks + b) * per_block
            window[to, at] = lines[i, first : first + per_block]
    turned = window[...].T
    packed[:width, :width] = matmul(turned, product[...])
    packed[:width, width:] = matmul(turned, window[...])
    last = 2 * n_blocks * per_block
    running = lines[0, last:]
    for i in range(1, n_x):
        running = running + lines[i, last:]
    packed[width:] = jnp.zeros((packed.shape[0] - width, 2 * width), F32)
    for b in range(n_blocks):
        packed[width : width + 1, b * LANES : (b + 1) * LANES] = running[b : b + 1]


def final_kernel(
    mine, other, residual, own, direction, block, first_rows, correction, ritz, metric, *, total
):
    n_rows, width = block.shape
    block[...] = own[:n_rows, width:]
    first_rows[...] = direction[:n_rows]
    ritz[...] = mine[:width, :width] + other[:width, :width]
    metric[...] = mine[:width, width:] + other[:width, width:]
    squares = mine[width : width + 1, :width] + other[width : width + 1, :width]
    scale = lax.rsqrt(squares / total + 1e-06)
    for b in range(width // LANES):
        at = slice(b * LANES, (b + 1) * LANES)
        correction[:, at] = residual[b * n_rows : (b + 1) * n_rows] * scale[:, at]


def on_device(
    hamiltonian_rows, current_block, correction_block, previous_block, ritz_values, mixing_coeffs
):
    n_z, n_x, n_c = (lax.axis_size(a) for a in ("row_0", "row_1", "col"))
    own_len, width = current_block.shape
    n_rows = hamiltonian_rows.shape[2]
    n_blocks = width // LANES
    window_total = n_rows * n_z * n_x * n_c
    per_block = n_z * n_rows
    n_lines = n_blocks * n_rows
    core = lax.axis_index("col")
    sizes = dict(n_rows=n_rows, n_blocks=n_blocks)

    tile = hamiltonian_rows.reshape(n_z, n_x, n_rows, n_c * own_len)
    tile = tile.transpose(1, 0, 2, 3).reshape(n_x * per_block, n_c * own_len)
    tile, correction_block = lax.optimization_barrier((tile, correction_block))

    own, direction = call(
        mix_kernel,
        "mix",
        (shape(own_len, 2 * width), shape(n_rows, width)),
        current_block,
        correction_block,
        previous_block,
        mixing_coeffs,
    )
    other = swap_cores(own)
    scaled_rows = current_block[:n_rows] * ritz_values[None, :]

    own_tile = lax.dynamic_slice_in_dim(tile, core * own_len, own_len, 1)
    n_sum = 2 * n_blocks * per_block
    partial, scaled, block_lines = call(
        partial_kernel,
        "partial",
        (shape(n_x, n_sum, LANES), shape(n_lines, LANES), shape(n_lines, LANES)),
        core.reshape(1),
        tile,
        other,
        matmul(own_tile, own),
        scaled_rows,
        own,
        in_spaces=[pltpu.SMEM] + [pltpu.VMEM] * 5,
    )

    by_x = exchange(partial, "row_1")
    slots = call(
        functools.partial(sum_x_kernel, **sizes),
        "sum_x",
        shape(n_z, 2 * n_lines, LANES),
        by_x,
        scratch=[pltpu.VMEM((n_sum, LANES), F32)],
    )
    by_z = exchange(slots, "row_0")
    residual, mine = call(
        functools.partial(residual_kernel, **sizes),
        "residual",
        (shape(n_lines, LANES), shape(n_z, 3, n_lines, LANES)),
        by_z,
        scaled,
        block_lines,
    )

    copies = call(
        functools.partial(gather_kernel, **sizes),
        "gather",
        shape(n_x, 2 * n_z * n_lines + padded(n_blocks), LANES),
        exchange(mine, "row_0"),
    )
    lines = exchange(copies, "row_1")
    packed = call(
        functools.partial(own_kernel, n_blocks=n_blocks, per_block=per_block),
        "own_grams",
        shape(width + SUBLANES, 2 * width),
        lines,
        scratch=[pltpu.VMEM((n_x * per_block, width), F32)] * 2,
    )
    return call(
        functools.partial(final_kernel, total=window_total),
        "final",
        (shape(n_rows, width),) * 3 + (shape(width, width),) * 2,
        packed,
        swap_cores(packed),
        residual,
        own,
        direction,
    )


def solution(mesh):
    finer = Mesh(
        mesh.devices.reshape(mesh.shape["chan"], 16, 8, mesh.shape["col"]),
        ("chan", "row_0", "row_1", "col"),
    )
    in_specs = (
        P("chan", "col", None, ROW),
        P(CHAN_ROW_COL, None),
        P(CHAN_ROW_COL, None),
        P(CHAN_ROW_COL, None),
        P("chan"),
        P("chan", None),
    )
    out_specs = (
        P(CHAN_ROW_COL, None),
        P(CHAN_ROW_COL, None),
        P(CHAN_ROW_COL, None),
        P("chan", None),
        P("chan", None),
    )
    return jax.shard_map(
        on_device, mesh=finer, in_specs=in_specs, out_specs=out_specs, check_vma=False
    )
```

```python
import functools

import jax
import jax.numpy as jnp
from jax import lax
from jax.experimental import pallas as pl
from jax.experimental.pallas import tpu as pltpu
from jax.sharding import Mesh
from jax.sharding import PartitionSpec as P

ROW = ("row_0", "row_1")
CHAN_ROW_COL = ("chan", "row_0", "row_1", "col")
LANES = 128
SUBLANES = 8
VMEM_BYTES = 8 * 2**20
F32 = jnp.float32


def shape(*dims):
    return jax.ShapeDtypeStruct(dims, F32)


def exchange(blocks, axis):
    return lax.all_to_all(blocks, axis, 0, 0, tiled=True)


def swap_cores(shard):
    return lax.ppermute(shard, "col", [(0, 1), (1, 0)])


def matmul(left, right):
    return jnp.dot(left, right, preferred_element_type=F32, precision=lax.Precision.HIGHEST)


def call(kernel, name, out_shape, *args, in_spaces=None, scratch=()):
    spaces = in_spaces or [pltpu.VMEM] * len(args)
    resident = pl.BlockSpec(memory_space=pltpu.VMEM)
    return pl.pallas_call(
        kernel,
        in_specs=[pl.BlockSpec(memory_space=space) for space in spaces],
        out_specs=jax.tree.map(lambda _: resident, out_shape),
        out_shape=out_shape,
        scratch_shapes=scratch,
        compiler_params=pltpu.CompilerParams(vmem_limit_bytes=VMEM_BYTES),
        name=name,
    )(*args)


def both_cores(shard):
    return lax.all_gather(shard, "col")


def padded(count):
    return -(-count // SUBLANES) * SUBLANES


def mix_kernel(x, w, p, c, own, direction):
    width = x.shape[1]
    total = matmul(w[...], c[width : 2 * width]) + matmul(p[...], c[2 * width :])
    direction[...] = total[: direction.shape[0]]
    own[:, :width] = x[...]
    own[:, width:] = total + matmul(x[...], c[:width])


def partial_kernel(
    core, tile, other, part, scaled, own, out, scaled_lines, block_lines
):
    n_x = out.shape[0]
    n_rows, width = scaled.shape
    length = other.shape[0]
    per_x = part.shape[0] // n_x
    n_blocks = width // LANES
    for b in range(n_blocks):
        at = slice(b * LANES, (b + 1) * LANES)
        scaled_lines[b * n_rows : (b + 1) * n_rows] = scaled[:, at]
        block_lines[b * n_rows : (b + 1) * n_rows] = own[
            :n_rows, width + b * LANES : width + (b + 1) * LANES
        ]

    def finish(first):
        total = part[...] + matmul(tile[:, first : first + length], other[...])
        for i in range(n_x):
            for b in range(2 * n_blocks):
                out[i, b * per_x : (b + 1) * per_x] = total[
                    i * per_x : (i + 1) * per_x, b * LANES : (b + 1) * LANES
                ]

    @pl.when(core[0] == 0)
    def _():
        finish(length)

    @pl.when(core[0] != 0)
    def _():
        finish(0)


def sum_x_kernel(by_x, out, total, *, n_rows, n_blocks):
    n_x = by_x.shape[0]
    n_z = out.shape[0]
    running = by_x[0]
    for i in range(1, n_x):
        running = running + by_x[i]
    total[...] = running
    for z in range(n_z):
        for b in range(2 * n_blocks):
            first = (b * n_z + z) * n_rows
            out[z, b * n_rows : (b + 1) * n_rows] = total[first : first + n_rows]


def residual_kernel(by_z, scaled, lines, residual, out, *, n_rows, n_blocks):
    n_lines = n_blocks * n_rows
    running = by_z[0]
    for z in range(1, by_z.shape[0]):
        running = running + by_z[z]
    rest = running[:n_lines] - scaled[...]
    residual[...] = rest
    squares = rest * rest
    out[0, 0] = running[n_lines:]
    out[0, 1] = lines[...]
    out[0, 2] = jnp.zeros((n_lines, LANES), F32)
    for b in range(n_blocks):
        at = slice(b * n_rows, (b + 1) * n_rows)
        out[0, 2, b : b + 1] = jnp.sum(squares[at], axis=0, keepdims=True)
    for z in range(1, out.shape[0]):
        out[z] = out[0]


def gather_kernel(by_z, out, *, n_rows, n_blocks):
    n_z = by_z.shape[0]
    n_lines = n_blocks * n_rows
    for z in range(n_z):
        for part in range(2):
            for b in range(n_blocks):
                first = ((part * n_blocks + b) * n_z + z) * n_rows
                out[0, first : first + n_rows] = by_z[z, part, b * n_rows : (b + 1) * n_rows]
    running = by_z[0, 2]
    for z in range(1, n_z):
        running = running + by_z[z, 2]
    last = 2 * n_z * n_lines
    out[0, last:] = jnp.zeros((out.shape[1] - last, LANES), F32)
    out[0, last : last + n_blocks] = running[:n_blocks]
    for i in range(1, out.shape[0]):
        out[i] = out[0]


def own_kernel(lines, packed, product, window, *, n_blocks, per_block):
    n_x = lines.shape[0]
    width = product.shape[1]
    for i in range(n_x):
        to = slice(i * per_block, (i + 1) * per_block)
        for b in range(n_blocks):
            at = slice(b * LANES, (b + 1) * LANES)
            product[to, at] = lines[i, b * per_block : (b + 1) * per_block]
            first = (n_blocks + b) * per_block
            window[to, at] = lines[i, first : first + per_block]
    turned = window[...].T
    ritz = matmul(turned, product[...])
    metric = matmul(turned, window[...])
    at = n_blocks * width
    for b in range(n_blocks):
        lanes = slice(b * LANES, (b + 1) * LANES)
        packed[b * width : (b + 1) * width] = ritz[:, lanes]
        packed[at : at + (b + 1) * LANES] = metric[: (b + 1) * LANES, lanes]
        at += (b + 1) * LANES
    last = 2 * n_blocks * per_block
    running = lines[0, last:]
    for i in range(1, n_x):
        running = running + lines[i, last:]
    packed[at:] = running


def final_kernel(
    packed, residual, own, direction, block, first_rows, correction, ritz, metric, *, total
):
    n_rows, width = block.shape
    n_blocks = width // LANES
    block[...] = own[:n_rows, width:]
    first_rows[...] = direction[:n_rows]

    def both(first, count):
        return packed[0, first : first + count] + packed[1, first : first + count]

    at = n_blocks * width
    for b in range(n_blocks):
        lanes = slice(b * LANES, (b + 1) * LANES)
        ritz[:, lanes] = both(b * width, width)
        for r in range(b + 1):
            rows = slice(r * LANES, (r + 1) * LANES)
            piece = both(at + r * LANES, LANES)
            metric[rows, lanes] = piece
            if r != b:
                metric[lanes, rows] = piece.T
        at += (b + 1) * LANES
    scale = lax.rsqrt(both(at, n_blocks) / total + 1e-06)
    for b in range(n_blocks):
        lanes = slice(b * LANES, (b + 1) * LANES)
        correction[:, lanes] = residual[b * n_rows : (b + 1) * n_rows] * scale[b : b + 1]


def on_device(
    hamiltonian_rows, current_block, correction_block, previous_block, ritz_values, mixing_coeffs
):
    n_z, n_x, n_c = (lax.axis_size(a) for a in ("row_0", "row_1", "col"))
    own_len, width = current_block.shape
    n_rows = hamiltonian_rows.shape[2]
    n_blocks = width // LANES
    window_total = n_rows * n_z * n_x * n_c
    per_block = n_z * n_rows
    n_lines = n_blocks * n_rows
    core = lax.axis_index("col")
    sizes = dict(n_rows=n_rows, n_blocks=n_blocks)

    tile = hamiltonian_rows.reshape(n_z, n_x, n_rows, n_c * own_len)
    tile = tile.transpose(1, 0, 2, 3).reshape(n_x * per_block, n_c * own_len)
    tile, correction_block = lax.optimization_barrier((tile, correction_block))

    own, direction = call(
        mix_kernel,
        "mix",
        (shape(own_len, 2 * width), shape(n_rows, width)),
        current_block,
        correction_block,
        previous_block,
        mixing_coeffs,
    )
    other = swap_cores(own)
    scaled_rows = current_block[:n_rows] * ritz_values[None, :]

    own_tile = lax.dynamic_slice_in_dim(tile, core * own_len, own_len, 1)
    n_sum = 2 * n_blocks * per_block
    partial, scaled, block_lines = call(
        partial_kernel,
        "partial",
        (shape(n_x, n_sum, LANES), shape(n_lines, LANES), shape(n_lines, LANES)),
        core.reshape(1),
        tile,
        other,
        matmul(own_tile, own),
        scaled_rows,
        own,
        in_spaces=[pltpu.SMEM] + [pltpu.VMEM] * 5,
    )

    by_x = exchange(partial, "row_1")
    slots = call(
        functools.partial(sum_x_kernel, **sizes),
        "sum_x",
        shape(n_z, 2 * n_lines, LANES),
        by_x,
        scratch=[pltpu.VMEM((n_sum, LANES), F32)],
    )
    by_z = exchange(slots, "row_0")
    residual, mine = call(
        functools.partial(residual_kernel, **sizes),
        "residual",
        (shape(n_lines, LANES), shape(n_z, 3, n_lines, LANES)),
        by_z,
        scaled,
        block_lines,
    )

    copies = call(
        functools.partial(gather_kernel, **sizes),
        "gather",
        shape(n_x, 2 * n_z * n_lines + padded(n_blocks), LANES),
        exchange(mine, "row_0"),
    )
    lines = exchange(copies, "row_1")
    packed_lines = n_blocks * width + n_blocks * (n_blocks + 1) // 2 * LANES + padded(n_blocks)
    packed = call(
        functools.partial(own_kernel, n_blocks=n_blocks, per_block=per_block),
        "own_grams",
        shape(packed_lines, LANES),
        lines,
        scratch=[pltpu.VMEM((n_x * per_block, width), F32)] * 2,
    )
    return call(
        functools.partial(final_kernel, total=window_total),
        "final",
        (shape(n_rows, width),) * 3 + (shape(width, width),) * 2,
        both_cores(packed),
        residual,
        own,
        direction,
    )


def solution(mesh):
    finer = Mesh(
        mesh.devices.reshape(mesh.shape["chan"], 16, 8, mesh.shape["col"]),
        ("chan", "row_0", "row_1", "col"),
    )
    in_specs = (
        P("chan", "col", None, ROW),
        P(CHAN_ROW_COL, None),
        P(CHAN_ROW_COL, None),
        P(CHAN_ROW_COL, None),
        P("chan"),
        P("chan", None),
    )
    out_specs = (
        P(CHAN_ROW_COL, None),
        P(CHAN_ROW_COL, None),
        P(CHAN_ROW_COL, None),
        P("chan", None),
        P("chan", None),
    )
    return jax.shard_map(
        on_device, mesh=finer, in_specs=in_specs, out_specs=out_specs, check_vma=False
    )
```

```python
import functools

import jax
import jax.numpy as jnp
from jax import lax
from jax.experimental import pallas as pl
from jax.experimental.pallas import tpu as pltpu
from jax.sharding import Mesh
from jax.sharding import PartitionSpec as P

ROW = ("row_0", "row_1")
CHAN_ROW_COL = ("chan", "row_0", "row_1", "col")
LANES = 128
SUBLANES = 8
VMEM_BYTES = 8 * 2**20
F32 = jnp.float32


def shape(*dims):
    return jax.ShapeDtypeStruct(dims, F32)


def exchange(blocks, axis):
    return lax.all_to_all(blocks, axis, 0, 0, tiled=True)


def swap_cores(shard):
    return lax.ppermute(shard, "col", [(0, 1), (1, 0)])


def matmul(left, right):
    return jnp.dot(left, right, preferred_element_type=F32, precision=lax.Precision.HIGHEST)


def call(kernel, name, out_shape, *args, in_spaces=None, scratch=(), cost=None):
    spaces = in_spaces or [pltpu.VMEM] * len(args)
    resident = pl.BlockSpec(memory_space=pltpu.VMEM)
    return pl.pallas_call(
        kernel,
        in_specs=[pl.BlockSpec(memory_space=space) for space in spaces],
        out_specs=jax.tree.map(lambda _: resident, out_shape),
        out_shape=out_shape,
        scratch_shapes=scratch,
        compiler_params=pltpu.CompilerParams(vmem_limit_bytes=VMEM_BYTES),
        cost_estimate=cost,
        name=name,
    )(*args)


def both_cores(shard):
    return lax.all_gather(shard, "col")


def padded(count):
    return -(-count // SUBLANES) * SUBLANES


def order_kernel(core, out):
    out[...] = jnp.full(out.shape, core[0].astype(F32))


def mix_kernel(order, x, w, p, c, own, direction):
    width = x.shape[1]
    total = matmul(w[...], c[width : 2 * width]) + matmul(p[...], c[2 * width :])
    direction[...] = total[: direction.shape[0]]
    own[:, :width] = x[...]
    own[:, width:] = total + matmul(x[...], c[:width])


def partial_kernel(
    core, tile, other, part, scaled, own, out, scaled_lines, block_lines
):
    n_x = out.shape[0]
    n_rows, width = scaled.shape
    length = other.shape[0]
    per_x = part.shape[0] // n_x
    n_blocks = width // LANES
    for b in range(n_blocks):
        at = slice(b * LANES, (b + 1) * LANES)
        scaled_lines[b * n_rows : (b + 1) * n_rows] = scaled[:, at]
        block_lines[b * n_rows : (b + 1) * n_rows] = own[
            :n_rows, width + b * LANES : width + (b + 1) * LANES
        ]

    def finish(first):
        total = part[...] + matmul(tile[:, first : first + length], other[...])
        for i in range(n_x):
            for b in range(2 * n_blocks):
                out[i, b * per_x : (b + 1) * per_x] = total[
                    i * per_x : (i + 1) * per_x, b * LANES : (b + 1) * LANES
                ]

    @pl.when(core[0] == 0)
    def _():
        finish(length)

    @pl.when(core[0] != 0)
    def _():
        finish(0)


def sum_x_kernel(by_x, out, total, *, n_rows, n_blocks):
    n_x = by_x.shape[0]
    n_z = out.shape[0]
    running = by_x[0]
    for i in range(1, n_x):
        running = running + by_x[i]
    total[...] = running
    for z in range(n_z):
        for b in range(2 * n_blocks):
            first = (b * n_z + z) * n_rows
            out[z, b * n_rows : (b + 1) * n_rows] = total[first : first + n_rows]


def residual_kernel(by_z, scaled, lines, residual, out, *, n_rows, n_blocks):
    n_lines = n_blocks * n_rows
    running = by_z[0]
    for z in range(1, by_z.shape[0]):
        running = running + by_z[z]
    rest = running[:n_lines] - scaled[...]
    residual[...] = rest
    squares = rest * rest
    for b in range(n_blocks):
        at = slice(b * n_rows, (b + 1) * n_rows)
        out[0, b] = running[n_lines + b * n_rows : n_lines + (b + 1) * n_rows]
        out[0, n_blocks + b] = lines[at]
        out[0, 2 * n_blocks, b : b + 1] = jnp.sum(squares[at], axis=0, keepdims=True)
    for z in range(1, out.shape[0]):
        out[z] = out[0]


def gather_kernel(by_z, out, *, n_rows, n_blocks):
    n_z = by_z.shape[0]
    for z in range(n_z):
        for piece in range(2 * n_blocks):
            first = (piece * n_z + z) * n_rows
            out[0, first : first + n_rows] = by_z[z, piece]
    running = by_z[0, 2 * n_blocks]
    for z in range(1, n_z):
        running = running + by_z[z, 2 * n_blocks]
    last = 2 * n_blocks * n_z * n_rows
    out[0, last:] = jnp.zeros((out.shape[1] - last, LANES), F32)
    out[0, last : last + n_blocks] = running[:n_blocks]
    for i in range(1, out.shape[0]):
        out[i] = out[0]


def own_kernel(lines, packed, product, window, *, n_blocks, per_block):
    n_x = lines.shape[0]
    width = product.shape[1]
    for i in range(n_x):
        to = slice(i * per_block, (i + 1) * per_block)
        for b in range(n_blocks):
            at = slice(b * LANES, (b + 1) * LANES)
            product[to, at] = lines[i, b * per_block : (b + 1) * per_block]
            first = (n_blocks + b) * per_block
            window[to, at] = lines[i, first : first + per_block]
    turned = window[...].T
    ritz = matmul(turned, product[...])
    metric = matmul(turned, window[...])
    at = n_blocks * width
    for b in range(n_blocks):
        lanes = slice(b * LANES, (b + 1) * LANES)
        packed[b * width : (b + 1) * width] = ritz[:, lanes]
        packed[at : at + (b + 1) * LANES] = metric[: (b + 1) * LANES, lanes]
        at += (b + 1) * LANES
    last = 2 * n_blocks * per_block
    running = lines[0, last:]
    for i in range(1, n_x):
        running = running + lines[i, last:]
    packed[at:] = running


def final_kernel(
    packed, residual, own, direction, block, first_rows, correction, ritz, metric, *, total
):
    n_rows, width = block.shape
    n_blocks = width // LANES
    block[...] = own[:n_rows, width:]
    first_rows[...] = direction[:n_rows]

    def both(first, count):
        return packed[0, first : first + count] + packed[1, first : first + count]

    at = n_blocks * width
    for b in range(n_blocks):
        lanes = slice(b * LANES, (b + 1) * LANES)
        ritz[:, lanes] = both(b * width, width)
        for r in range(b + 1):
            rows = slice(r * LANES, (r + 1) * LANES)
            piece = both(at + r * LANES, LANES)
            metric[rows, lanes] = piece
            if r != b:
                metric[lanes, rows] = piece.T
        at += (b + 1) * LANES
    scale = lax.rsqrt(both(at, n_blocks) / total + 1e-06)
    for b in range(n_blocks):
        lanes = slice(b * LANES, (b + 1) * LANES)
        correction[:, lanes] = residual[b * n_rows : (b + 1) * n_rows] * scale[b : b + 1]


def on_device(
    hamiltonian_rows, current_block, correction_block, previous_block, ritz_values, mixing_coeffs
):
    n_z, n_x, n_c = (lax.axis_size(a) for a in ("row_0", "row_1", "col"))
    own_len, width = current_block.shape
    n_rows = hamiltonian_rows.shape[2]
    n_blocks = width // LANES
    window_total = n_rows * n_z * n_x * n_c
    per_block = n_z * n_rows
    n_lines = n_blocks * n_rows
    core = lax.axis_index("col")
    sizes = dict(n_rows=n_rows, n_blocks=n_blocks)
    assert n_blocks == n_rows

    tile = hamiltonian_rows.reshape(n_z, n_x, n_rows, n_c * own_len)
    tile = tile.transpose(1, 0, 2, 3).reshape(n_x * per_block, n_c * own_len)

    own, direction = call(
        mix_kernel,
        "mix",
        (shape(own_len, 2 * width), shape(n_rows, width)),
        call(
            order_kernel,
            "order",
            shape(SUBLANES, LANES),
            core.reshape(1),
            in_spaces=[pltpu.SMEM],
            cost=pl.CostEstimate(flops=10**9, transcendentals=0, bytes_accessed=0),
        ),
        current_block,
        correction_block,
        previous_block,
        mixing_coeffs,
    )
    other = swap_cores(own)
    scaled_rows = current_block[:n_rows] * ritz_values[None, :]

    own_tile = lax.dynamic_slice_in_dim(tile, core * own_len, own_len, 1)
    n_sum = 2 * n_blocks * per_block
    partial, scaled, block_lines = call(
        partial_kernel,
        "partial",
        (shape(n_x, n_sum, LANES), shape(n_lines, LANES), shape(n_lines, LANES)),
        core.reshape(1),
        tile,
        other,
        matmul(own_tile, own),
        scaled_rows,
        own,
        in_spaces=[pltpu.SMEM] + [pltpu.VMEM] * 5,
    )

    by_x = exchange(partial, "row_1")
    slots = call(
        functools.partial(sum_x_kernel, **sizes),
        "sum_x",
        shape(n_z, 2 * n_lines, LANES),
        by_x,
        scratch=[pltpu.VMEM((n_sum, LANES), F32)],
    )
    by_z = exchange(slots, "row_0")
    residual, mine = call(
        functools.partial(residual_kernel, **sizes),
        "residual",
        (shape(n_lines, LANES), shape(n_z, 2 * n_blocks + 1, n_rows, LANES)),
        by_z,
        scaled,
        block_lines,
    )

    copies = call(
        functools.partial(gather_kernel, **sizes),
        "gather",
        shape(n_x, 2 * n_z * n_lines + padded(n_blocks), LANES),
        exchange(mine, "row_0"),
    )
    lines = exchange(copies, "row_1")
    packed_lines = n_blocks * width + n_blocks * (n_blocks + 1) // 2 * LANES + padded(n_blocks)
    packed = call(
        functools.partial(own_kernel, n_blocks=n_blocks, per_block=per_block),
        "own_grams",
        shape(packed_lines, LANES),
        lines,
        scratch=[pltpu.VMEM((n_x * per_block, width), F32)] * 2,
    )
    return call(
        functools.partial(final_kernel, total=window_total),
        "final",
        (shape(n_rows, width),) * 3 + (shape(width, width),) * 2,
        both_cores(packed),
        residual,
        own,
        direction,
    )


def solution(mesh):
    finer = Mesh(
        mesh.devices.reshape(mesh.shape["chan"], 16, 8, mesh.shape["col"]),
        ("chan", "row_0", "row_1", "col"),
    )
    in_specs = (
        P("chan", "col", None, ROW),
        P(CHAN_ROW_COL, None),
        P(CHAN_ROW_COL, None),
        P(CHAN_ROW_COL, None),
        P("chan"),
        P("chan", None),
    )
    out_specs = (
        P(CHAN_ROW_COL, None),
        P(CHAN_ROW_COL, None),
        P(CHAN_ROW_COL, None),
        P("chan", None),
        P("chan", None),
    )
    return jax.shard_map(
        on_device, mesh=finer, in_specs=in_specs, out_specs=out_specs, check_vma=False
    )
```

```python
import functools

import jax
import jax.numpy as jnp
from jax import lax
from jax.experimental import pallas as pl
from jax.experimental.pallas import tpu as pltpu
from jax.sharding import Mesh
from jax.sharding import PartitionSpec as P

ROW = ("row_0", "row_1")
CHAN_ROW_COL = ("chan", "row_0", "row_1", "col")
LANES = 128
SUBLANES = 8
VMEM_BYTES = 8 * 2**20
F32 = jnp.float32


def shape(*dims):
    return jax.ShapeDtypeStruct(dims, F32)


def exchange(blocks, axis):
    return lax.all_to_all(blocks, axis, 0, 0, tiled=True)


def swap_cores(shard):
    return lax.ppermute(shard, "col", [(0, 1), (1, 0)])


def matmul(left, right):
    return jnp.dot(left, right, preferred_element_type=F32, precision=lax.Precision.HIGHEST)


def call(kernel, name, out_shape, *args, in_spaces=None, scratch=(), cost=None):
    spaces = in_spaces or [pltpu.VMEM] * len(args)
    resident = pl.BlockSpec(memory_space=pltpu.VMEM)
    return pl.pallas_call(
        kernel,
        in_specs=[pl.BlockSpec(memory_space=space) for space in spaces],
        out_specs=jax.tree.map(lambda _: resident, out_shape),
        out_shape=out_shape,
        scratch_shapes=scratch,
        compiler_params=pltpu.CompilerParams(vmem_limit_bytes=VMEM_BYTES),
        cost_estimate=cost,
        name=name,
    )(*args)


def both_cores(shard):
    return lax.all_gather(shard, "col")


def padded(count):
    return -(-count // SUBLANES) * SUBLANES


def order_kernel(core, out):
    out[...] = jnp.full(out.shape, core[0].astype(F32))


def mix_kernel(order, x, w, p, c, own, direction):
    width = x.shape[1]
    total = matmul(w[...], c[width : 2 * width]) + matmul(p[...], c[2 * width :])
    direction[...] = total[: direction.shape[0]]
    own[:, :width] = x[...]
    own[:, width:] = total + matmul(x[...], c[:width])


def partial_kernel(
    core, tile, other, part, scaled, own, out, scaled_lines, block_lines
):
    n_x = out.shape[0]
    n_rows, width = scaled.shape
    length = other.shape[0]
    per_x = part.shape[0] // n_x
    n_blocks = width // LANES
    for b in range(n_blocks):
        at = slice(b * LANES, (b + 1) * LANES)
        scaled_lines[b * n_rows : (b + 1) * n_rows] = scaled[:, at]
        block_lines[b * n_rows : (b + 1) * n_rows] = own[
            :n_rows, width + b * LANES : width + (b + 1) * LANES
        ]

    def finish(first):
        total = part[...] + matmul(tile[:, first : first + length], other[...])
        for i in range(n_x):
            for b in range(2 * n_blocks):
                out[i, b * per_x : (b + 1) * per_x] = total[
                    i * per_x : (i + 1) * per_x, b * LANES : (b + 1) * LANES
                ]

    @pl.when(core[0] == 0)
    def _():
        finish(length)

    @pl.when(core[0] != 0)
    def _():
        finish(0)


def sum_x_kernel(by_x, out, total, *, n_rows, n_blocks):
    n_x = by_x.shape[0]
    n_z = out.shape[0]
    running = by_x[0]
    for i in range(1, n_x):
        running = running + by_x[i]
    total[...] = running
    for z in range(n_z):
        for b in range(2 * n_blocks):
            first = (b * n_z + z) * n_rows
            out[z, b * n_rows : (b + 1) * n_rows] = total[first : first + n_rows]


def residual_kernel(by_z, scaled, lines, residual, out, *, n_rows, n_blocks):
    n_lines = n_blocks * n_rows
    running = by_z[0]
    for z in range(1, by_z.shape[0]):
        running = running + by_z[z]
    rest = running[:n_lines] - scaled[...]
    residual[...] = rest
    squares = rest * rest
    out[0, 0] = running[n_lines:]
    out[0, 1] = lines[...]
    out[0, 2] = jnp.zeros((n_lines, LANES), F32)
    for b in range(n_blocks):
        at = slice(b * n_rows, (b + 1) * n_rows)
        out[0, 2, b : b + 1] = jnp.sum(squares[at], axis=0, keepdims=True)
    for z in range(1, out.shape[0]):
        out[z] = out[0]


def gather_kernel(by_z, out, *, n_rows, n_blocks):
    n_z = by_z.shape[0]
    n_lines = n_blocks * n_rows
    for z in range(n_z):
        for part in range(2):
            for b in range(n_blocks):
                first = ((part * n_blocks + b) * n_z + z) * n_rows
                out[0, first : first + n_rows] = by_z[z, part, b * n_rows : (b + 1) * n_rows]
    running = by_z[0, 2]
    for z in range(1, n_z):
        running = running + by_z[z, 2]
    last = 2 * n_z * n_lines
    out[0, last:] = jnp.zeros((out.shape[1] - last, LANES), F32)
    out[0, last : last + n_blocks] = running[:n_blocks]
    for i in range(1, out.shape[0]):
        out[i] = out[0]


def own_kernel(lines, packed, product, window, *, n_blocks, per_block):
    n_x = lines.shape[0]
    width = product.shape[1]
    for i in range(n_x):
        to = slice(i * per_block, (i + 1) * per_block)
        for b in range(n_blocks):
            at = slice(b * LANES, (b + 1) * LANES)
            product[to, at] = lines[i, b * per_block : (b + 1) * per_block]
            first = (n_blocks + b) * per_block
            window[to, at] = lines[i, first : first + per_block]
    turned = window[...].T
    ritz = matmul(turned, product[...])
    metric = matmul(turned, window[...])
    at = n_blocks * width
    for b in range(n_blocks):
        lanes = slice(b * LANES, (b + 1) * LANES)
        packed[b * width : (b + 1) * width] = ritz[:, lanes]
        packed[at : at + (b + 1) * LANES] = metric[: (b + 1) * LANES, lanes]
        at += (b + 1) * LANES
    last = 2 * n_blocks * per_block
    running = lines[0, last:]
    for i in range(1, n_x):
        running = running + lines[i, last:]
    packed[at:] = running


def final_kernel(
    packed, residual, own, direction, block, first_rows, correction, ritz, metric, *, total
):
    n_rows, width = block.shape
    n_blocks = width // LANES
    block[...] = own[:n_rows, width:]
    first_rows[...] = direction[:n_rows]

    def both(first, count):
        return packed[0, first : first + count] + packed[1, first : first + count]

    at = n_blocks * width
    for b in range(n_blocks):
        lanes = slice(b * LANES, (b + 1) * LANES)
        ritz[:, lanes] = both(b * width, width)
        for r in range(b + 1):
            rows = slice(r * LANES, (r + 1) * LANES)
            piece = both(at + r * LANES, LANES)
            metric[rows, lanes] = piece
            if r != b:
                metric[lanes, rows] = piece.T
        at += (b + 1) * LANES
    scale = lax.rsqrt(both(at, n_blocks) / total + 1e-06)
    for b in range(n_blocks):
        lanes = slice(b * LANES, (b + 1) * LANES)
        correction[:, lanes] = residual[b * n_rows : (b + 1) * n_rows] * scale[b : b + 1]


def on_device(
    hamiltonian_rows, current_block, correction_block, previous_block, ritz_values, mixing_coeffs
):
    n_z, n_x, n_c = (lax.axis_size(a) for a in ("row_0", "row_1", "col"))
    own_len, width = current_block.shape
    n_rows = hamiltonian_rows.shape[2]
    n_blocks = width // LANES
    window_total = n_rows * n_z * n_x * n_c
    per_block = n_z * n_rows
    n_lines = n_blocks * n_rows
    core = lax.axis_index("col")
    sizes = dict(n_rows=n_rows, n_blocks=n_blocks)

    tile = hamiltonian_rows.reshape(n_z, n_x, n_rows, n_c * own_len)
    tile = tile.transpose(1, 0, 2, 3).reshape(n_x * per_block, n_c * own_len)

    own, direction = call(
        mix_kernel,
        "mix",
        (shape(own_len, 2 * width), shape(n_rows, width)),
        call(
            order_kernel,
            "order",
            shape(SUBLANES, LANES),
            core.reshape(1),
            in_spaces=[pltpu.SMEM],
            cost=pl.CostEstimate(flops=10**9, transcendentals=0, bytes_accessed=0),
        ),
        current_block,
        correction_block,
        previous_block,
        mixing_coeffs,
    )
    other = swap_cores(own)
    scaled_rows = current_block[:n_rows] * ritz_values[None, :]

    own_tile = lax.dynamic_slice_in_dim(tile, core * own_len, own_len, 1)
    n_sum = 2 * n_blocks * per_block
    partial, scaled, block_lines = call(
        partial_kernel,
        "partial",
        (shape(n_x, n_sum, LANES), shape(n_lines, LANES), shape(n_lines, LANES)),
        core.reshape(1),
        tile,
        other,
        matmul(own_tile, own),
        scaled_rows,
        own,
        in_spaces=[pltpu.SMEM] + [pltpu.VMEM] * 5,
    )

    by_x = exchange(partial, "row_1")
    slots = call(
        functools.partial(sum_x_kernel, **sizes),
        "sum_x",
        shape(n_z, 2 * n_lines, LANES),
        by_x,
        scratch=[pltpu.VMEM((n_sum, LANES), F32)],
    )
    by_z = exchange(slots, "row_0")
    residual, mine = call(
        functools.partial(residual_kernel, **sizes),
        "residual",
        (shape(n_lines, LANES), shape(n_z, 3, n_lines, LANES)),
        by_z,
        scaled,
        block_lines,
    )

    copies = call(
        functools.partial(gather_kernel, **sizes),
        "gather",
        shape(n_x, 2 * n_z * n_lines + padded(n_blocks), LANES),
        exchange(mine, "row_0"),
    )
    lines = exchange(copies, "row_1")
    packed_lines = n_blocks * width + n_blocks * (n_blocks + 1) // 2 * LANES + padded(n_blocks)
    packed = call(
        functools.partial(own_kernel, n_blocks=n_blocks, per_block=per_block),
        "own_grams",
        shape(packed_lines, LANES),
        lines,
        scratch=[pltpu.VMEM((n_x * per_block, width), F32)] * 2,
    )
    return call(
        functools.partial(final_kernel, total=window_total),
        "final",
        (shape(n_rows, width),) * 3 + (shape(width, width),) * 2,
        both_cores(packed),
        residual,
        own,
        direction,
    )


def solution(mesh):
    finer = Mesh(
        mesh.devices.reshape(mesh.shape["chan"], 16, 8, mesh.shape["col"]),
        ("chan", "row_0", "row_1", "col"),
    )
    in_specs = (
        P("chan", "col", None, ROW),
        P(CHAN_ROW_COL, None),
        P(CHAN_ROW_COL, None),
        P(CHAN_ROW_COL, None),
        P("chan"),
        P("chan", None),
    )
    out_specs = (
        P(CHAN_ROW_COL, None),
        P(CHAN_ROW_COL, None),
        P(CHAN_ROW_COL, None),
        P("chan", None),
        P("chan", None),
    )
    return jax.shard_map(
        on_device, mesh=finer, in_specs=in_specs, out_specs=out_specs, check_vma=False
    )
```

```python
import functools

import jax
import jax.numpy as jnp
from jax import lax
from jax.experimental import pallas as pl
from jax.experimental.pallas import tpu as pltpu
from jax.sharding import Mesh
from jax.sharding import PartitionSpec as P

ROW = ("row_0", "row_1")
CHAN_ROW_COL = ("chan", "row_0", "row_1", "col")
LANES = 128
SUBLANES = 8
VMEM_BYTES = 8 * 2**20
F32 = jnp.float32


def shape(*dims):
    return jax.ShapeDtypeStruct(dims, F32)


def exchange(blocks, axis):
    return lax.all_to_all(blocks, axis, 0, 0, tiled=True)


def swap_cores(shard):
    return lax.ppermute(shard, "col", [(0, 1), (1, 0)])


def matmul(left, right):
    return jnp.dot(left, right, preferred_element_type=F32, precision=lax.Precision.HIGHEST)


def call(kernel, name, out_shape, *args, in_spaces=None, scratch=()):
    spaces = in_spaces or [pltpu.VMEM] * len(args)
    resident = pl.BlockSpec(memory_space=pltpu.VMEM)
    return pl.pallas_call(
        kernel,
        in_specs=[pl.BlockSpec(memory_space=space) for space in spaces],
        out_specs=jax.tree.map(lambda _: resident, out_shape),
        out_shape=out_shape,
        scratch_shapes=scratch,
        compiler_params=pltpu.CompilerParams(vmem_limit_bytes=VMEM_BYTES),
        name=name,
    )(*args)


def both_cores(shard):
    return lax.all_gather(shard, "col")


def padded(count):
    return -(-count // SUBLANES) * SUBLANES


def mix_kernel(x, w, p, c, own, direction):
    width = x.shape[1]
    total = matmul(w[...], c[width : 2 * width]) + matmul(p[...], c[2 * width :])
    direction[...] = total[: direction.shape[0]]
    own[:, :width] = x[...]
    own[:, width:] = total + matmul(x[...], c[:width])


def partial_kernel(
    core, tile, other, part, scaled, own, out, scaled_lines, block_lines
):
    n_x = out.shape[0]
    n_rows, width = scaled.shape
    length = other.shape[0]
    per_x = part.shape[0] // n_x
    n_blocks = width // LANES
    for b in range(n_blocks):
        at = slice(b * LANES, (b + 1) * LANES)
        scaled_lines[b * n_rows : (b + 1) * n_rows] = scaled[:, at]
        block_lines[b * n_rows : (b + 1) * n_rows] = own[
            :n_rows, width + b * LANES : width + (b + 1) * LANES
        ]

    def finish(first):
        total = part[...] + matmul(tile[:, first : first + length], other[...])
        for i in range(n_x):
            for b in range(2 * n_blocks):
                out[i, b * per_x : (b + 1) * per_x] = total[
                    i * per_x : (i + 1) * per_x, b * LANES : (b + 1) * LANES
                ]

    @pl.when(core[0] == 0)
    def _():
        finish(length)

    @pl.when(core[0] != 0)
    def _():
        finish(0)


def sum_x_kernel(by_x, out, total, *, n_rows, n_blocks):
    n_x = by_x.shape[0]
    n_z = out.shape[0]
    running = by_x[0]
    for i in range(1, n_x):
        running = running + by_x[i]
    total[...] = running
    for z in range(n_z):
        for b in range(2 * n_blocks):
            first = (b * n_z + z) * n_rows
            out[z, b * n_rows : (b + 1) * n_rows] = total[first : first + n_rows]


def residual_kernel(by_z, scaled, lines, residual, out, *, n_rows, n_blocks):
    n_lines = n_blocks * n_rows
    running = by_z[0]
    for z in range(1, by_z.shape[0]):
        running = running + by_z[z]
    rest = running[:n_lines] - scaled[...]
    residual[...] = rest
    squares = rest * rest
    for b in range(n_blocks):
        at = slice(b * n_rows, (b + 1) * n_rows)
        out[0, b] = running[n_lines + b * n_rows : n_lines + (b + 1) * n_rows]
        out[0, n_blocks + b] = lines[at]
        out[0, 2 * n_blocks, b : b + 1] = jnp.sum(squares[at], axis=0, keepdims=True)
    for z in range(1, out.shape[0]):
        out[z] = out[0]


def gather_kernel(by_z, out, *, n_rows, n_blocks):
    n_z = by_z.shape[0]
    for z in range(n_z):
        for piece in range(2 * n_blocks):
            first = (piece * n_z + z) * n_rows
            out[0, first : first + n_rows] = by_z[z, piece]
    running = by_z[0, 2 * n_blocks]
    for z in range(1, n_z):
        running = running + by_z[z, 2 * n_blocks]
    last = 2 * n_blocks * n_z * n_rows
    out[0, last:] = jnp.zeros((out.shape[1] - last, LANES), F32)
    out[0, last : last + n_blocks] = running[:n_blocks]
    for i in range(1, out.shape[0]):
        out[i] = out[0]


def own_kernel(lines, packed, product, window, *, n_blocks, per_block):
    n_x = lines.shape[0]
    width = product.shape[1]
    for i in range(n_x):
        to = slice(i * per_block, (i + 1) * per_block)
        for b in range(n_blocks):
            at = slice(b * LANES, (b + 1) * LANES)
            product[to, at] = lines[i, b * per_block : (b + 1) * per_block]
            first = (n_blocks + b) * per_block
            window[to, at] = lines[i, first : first + per_block]
    turned = window[...].T
    ritz = matmul(turned, product[...])
    metric = matmul(turned, window[...])
    at = n_blocks * width
    for b in range(n_blocks):
        lanes = slice(b * LANES, (b + 1) * LANES)
        packed[b * width : (b + 1) * width] = ritz[:, lanes]
        packed[at : at + (b + 1) * LANES] = metric[: (b + 1) * LANES, lanes]
        at += (b + 1) * LANES
    last = 2 * n_blocks * per_block
    running = lines[0, last:]
    for i in range(1, n_x):
        running = running + lines[i, last:]
    packed[at:] = running


def final_kernel(
    packed, residual, own, direction, block, first_rows, correction, ritz, metric, *, total
):
    n_rows, width = block.shape
    n_blocks = width // LANES
    block[...] = own[:n_rows, width:]
    first_rows[...] = direction[:n_rows]

    def both(first, count):
        return packed[0, first : first + count] + packed[1, first : first + count]

    at = n_blocks * width
    for b in range(n_blocks):
        lanes = slice(b * LANES, (b + 1) * LANES)
        ritz[:, lanes] = both(b * width, width)
        for r in range(b + 1):
            rows = slice(r * LANES, (r + 1) * LANES)
            piece = both(at + r * LANES, LANES)
            metric[rows, lanes] = piece
            if r != b:
                metric[lanes, rows] = piece.T
        at += (b + 1) * LANES
    scale = lax.rsqrt(both(at, n_blocks) / total + 1e-06)
    for b in range(n_blocks):
        lanes = slice(b * LANES, (b + 1) * LANES)
        correction[:, lanes] = residual[b * n_rows : (b + 1) * n_rows] * scale[b : b + 1]


def on_device(
    hamiltonian_rows, current_block, correction_block, previous_block, ritz_values, mixing_coeffs
):
    n_z, n_x, n_c = (lax.axis_size(a) for a in ("row_0", "row_1", "col"))
    own_len, width = current_block.shape
    n_rows = hamiltonian_rows.shape[2]
    n_blocks = width // LANES
    window_total = n_rows * n_z * n_x * n_c
    per_block = n_z * n_rows
    n_lines = n_blocks * n_rows
    core = lax.axis_index("col")
    sizes = dict(n_rows=n_rows, n_blocks=n_blocks)
    assert n_blocks == n_rows

    tile = hamiltonian_rows.reshape(n_z, n_x, n_rows, n_c * own_len)
    tile = tile.transpose(1, 0, 2, 3).reshape(n_x * per_block, n_c * own_len)
    tile, correction_block = lax.optimization_barrier((tile, correction_block))

    own, direction = call(
        mix_kernel,
        "mix",
        (shape(own_len, 2 * width), shape(n_rows, width)),
        current_block,
        correction_block,
        previous_block,
        mixing_coeffs,
    )
    other = swap_cores(own)
    scaled_rows = current_block[:n_rows] * ritz_values[None, :]

    own_tile = lax.dynamic_slice_in_dim(tile, core * own_len, own_len, 1)
    n_sum = 2 * n_blocks * per_block
    partial, scaled, block_lines = call(
        partial_kernel,
        "partial",
        (shape(n_x, n_sum, LANES), shape(n_lines, LANES), shape(n_lines, LANES)),
        core.reshape(1),
        tile,
        other,
        matmul(own_tile, own),
        scaled_rows,
        own,
        in_spaces=[pltpu.SMEM] + [pltpu.VMEM] * 5,
    )

    by_x = exchange(partial, "row_1")
    slots = call(
        functools.partial(sum_x_kernel, **sizes),
        "sum_x",
        shape(n_z, 2 * n_lines, LANES),
        by_x,
        scratch=[pltpu.VMEM((n_sum, LANES), F32)],
    )
    by_z = exchange(slots, "row_0")
    residual, mine = call(
        functools.partial(residual_kernel, **sizes),
        "residual",
        (shape(n_lines, LANES), shape(n_z, 2 * n_blocks + 1, n_rows, LANES)),
        by_z,
        scaled,
        block_lines,
    )

    copies = call(
        functools.partial(gather_kernel, **sizes),
        "gather",
        shape(n_x, 2 * n_z * n_lines + padded(n_blocks), LANES),
        exchange(mine, "row_0"),
    )
    lines = exchange(copies, "row_1")
    packed_lines = n_blocks * width + n_blocks * (n_blocks + 1) // 2 * LANES + padded(n_blocks)
    packed = call(
        functools.partial(own_kernel, n_blocks=n_blocks, per_block=per_block),
        "own_grams",
        shape(packed_lines, LANES),
        lines,
        scratch=[pltpu.VMEM((n_x * per_block, width), F32)] * 2,
    )
    return call(
        functools.partial(final_kernel, total=window_total),
        "final",
        (shape(n_rows, width),) * 3 + (shape(width, width),) * 2,
        both_cores(packed),
        residual,
        own,
        direction,
    )


def solution(mesh):
    finer = Mesh(
        mesh.devices.reshape(mesh.shape["chan"], 16, 8, mesh.shape["col"]),
        ("chan", "row_0", "row_1", "col"),
    )
    in_specs = (
        P("chan", "col", None, ROW),
        P(CHAN_ROW_COL, None),
        P(CHAN_ROW_COL, None),
        P(CHAN_ROW_COL, None),
        P("chan"),
        P("chan", None),
    )
    out_specs = (
        P(CHAN_ROW_COL, None),
        P(CHAN_ROW_COL, None),
        P(CHAN_ROW_COL, None),
        P("chan", None),
        P("chan", None),
    )
    return jax.shard_map(
        on_device, mesh=finer, in_specs=in_specs, out_specs=out_specs, check_vma=False
    )
```
